32 devices in a mesh: gz: 8 (over z, x), gy: 4 (over y, core).
Axes of the slice: x: 2, y: 2, z: 4, core: 2. Of those that a mesh axis runs over, the one named last changes fastest.
Arguments:
- ranks: float32 [64, 64, 512], P('gz', 'gy'), may hold values from 1 to 2
- seeds: float32 [3, 64, 64, 512], P(None, 'gz', 'gy'), may hold values from 0.25 to 1
- flags: int32 [64, 64, 512], P('gz', 'gy'), may hold values 0 or 1
Outputs:
- states: int32 [64, 64, 512], P('gz', 'gy')
- undecided: int32 [3], replicated
The draws below stay inside these ranges and needn't reach their ends.
All inputs are finite; a program needn't handle non-finite values. No bound on the sum of `flags` on one device may be relied on, other than what follows from the above.
Results may differ from the reference program's by a relative error of at most 0.000001.
Values sent between devices are 32-bit elements; how exact they have to be, the bound alone decides.
No kernel may reach another device: no remote copies, remote signals or barrier semaphores. Data moves between devices by JAX's collectives and lax.ppermute only.
A program may use at most 64 MiB of HBM per device.

```python
import math
import jax
import jax.numpy as jnp

NX = 512
ROUNDS = 3
NY = 64
NZ = 64


def set_ends(drawn, key, low, top_value):
    extent = drawn.shape
    spot = [jax.random.randint(jax.random.fold_in(key, axis), (), 0, extent[axis]) for axis in range(len(extent))]
    drawn = drawn.at[tuple(spot)].set(low)
    longest = extent.index(max(extent))
    spot[longest] = (spot[longest] + 1) % extent[longest]
    return drawn.at[tuple(spot)].set(top_value)


def steps_of(key, dims, pieces, smallest, largest):
    def one(dim, parts):
        draws = jax.random.uniform(jax.random.fold_in(jax.random.fold_in(key, 6), dim), (parts,), jnp.float32, smallest / len(pieces), largest / len(pieces))
        return jnp.repeat(jnp.exp(draws), dims[dim] // parts).reshape((-1,) + (1,) * (len(dims) - dim - 1))

    level = one(*pieces[0])
    for cut in pieces[1:]:
        level = level * one(*cut)
    return level


def setup_inputs(seed: int = 0) -> dict:
    keys = jax.random.split(jax.random.key(seed), 4)
    return {
        "ranks": jnp.clip(1.0 + 1.0 * jax.random.uniform(keys[0], (NZ, NY, NX), jnp.float32) ** steps_of(keys[0], (NZ, NY, NX), ((0, 8), (1, 4)), -0.2, 0.2), 1.0, 2.0),
        "seeds": jnp.clip(jnp.exp(math.log(1.0) - 1.3862944 * jax.random.uniform(keys[1], (3, NZ, NY, NX), jnp.float32) ** steps_of(keys[1], (3, NZ, NY, NX), ((1, 8), (2, 4)), -0.2, 0.2)), 0.25, 1.0),
        "flags": set_ends((jax.random.randint(keys[2], (NZ, NY, NX), 0, 8) < 1).astype(jnp.int32), jax.random.fold_in(keys[2], 1), 0, 1),
    }


def beside_all(ext, fill):
    wide = jnp.pad(ext, ((0, 0), (0, 0), (1, 1)), constant_values=fill)
    return [wide[1:-1, 1:-1, 2:], wide[1:-1, 1:-1, :-2], wide[1:-1, 2:, 1:-1],
            wide[1:-1, :-2, 1:-1], wide[2:, 1:-1, 1:-1], wide[:-2, 1:-1, 1:-1]]


def cycle(field, width, fill):
    return jnp.pad(field, ((width, width), (width, width), (0, 0)), constant_values=fill)


def bit_of(bits, number):
    return (bits // (2 ** number)) % 2


def select(packed_ext, bits):
    center = packed_ext[1:-1, 1:-1]
    values = beside_all(packed_ext, -3.0)
    nearest = jnp.full(center.shape, -3.0, center.dtype)
    for direction in range(6):
        linked = (bit_of(bits, direction) + bit_of(bits, direction + 6)) > 0
        nearest = jnp.maximum(nearest, jnp.where(linked, values[direction], -3.0))
    return ((center >= 0) & (center > nearest)).astype(jnp.int32)


def finer(coarse_ext, bits):
    values = beside_all(coarse_ext, 0)
    hit = jnp.zeros(bits.shape, jnp.int32)
    for direction in range(6):
        hit = hit + bit_of(bits, direction) * values[direction]
    return hit


def reference(ranks, seeds, flags):
    nz, ny, nx = ranks.shape
    zpos = jnp.arange(nz, dtype=jnp.int32)[:, None, None]
    ypos = jnp.arange(ny, dtype=jnp.int32)[None, :, None]
    xpos = jnp.arange(nx, dtype=jnp.int32)[None, None, :]
    zero = jnp.zeros((), jnp.float32)
    c0 = jnp.where(xpos < nx - 1, seeds[0], zero).astype(jnp.float32)
    c2 = jnp.where(ypos < ny - 1, seeds[1], zero).astype(jnp.float32)
    c4 = jnp.where(zpos < nz - 1, seeds[2], zero).astype(jnp.float32)
    c1 = jnp.pad(c0[:, :, :-1], ((0, 0), (0, 0), (1, 0)))
    c3 = jnp.pad(c2[:, :-1], ((0, 0), (1, 0), (0, 0)))
    c5 = jnp.pad(c4[:-1], ((1, 0), (0, 0), (0, 0)))
    couplings = [c0, c1, c2, c3, c4, c5]
    rowmax = c0
    for item in couplings[1:]:
        rowmax = jnp.maximum(rowmax, item)
    others = beside_all(cycle(rowmax, 1, 0.0), 0.0)
    bits = jnp.zeros(ranks.shape, jnp.int32)
    scale = jnp.ones(ranks.shape, jnp.float32)
    two = jnp.ones((), jnp.float32) * 2.0
    one = jnp.ones((), jnp.float32)
    for direction in range(6):
        cost = couplings[direction]
        depends = ((cost > 0) & (2.0 * cost >= rowmax)).astype(jnp.int32)
        feeds = ((cost > 0) & (2.0 * cost >= others[direction])).astype(jnp.int32)
        bits = bits + depends * (2 ** direction) + feeds * (2 ** (direction + 6))
        scale = scale * jnp.where(feeds == 1, two, one)
    measure = (ranks * scale).astype(jnp.float32)
    state = flags
    totals = []
    for step in range(ROUNDS):
        packed = jnp.where(state == 0, measure, jnp.where(state == 2, -2.0, -1.0)).astype(jnp.float32)
        coarse = select(cycle(packed, 1, 0.0), bits)
        hit = finer(cycle(coarse, 1, 0), bits)
        state = jnp.where(coarse == 1, 2, jnp.where((state == 0) & (hit > 0), 1, state)).astype(jnp.int32)
        totals.append(jnp.sum((state == 0).astype(jnp.int32)))
    return state, jnp.stack(totals).astype(jnp.int32)
```

```python
import functools

import jax
import jax.numpy as jnp
from jax import lax
from jax.experimental import pallas as pl
from jax.experimental.pallas import tpu as pltpu
from jax.sharding import PartitionSpec as P

ROUNDS = 3
H = 2 * ROUNDS
T = 8
BIG = 3.0e38


def whole():
    return pl.BlockSpec(memory_space=pltpu.VMEM)


def pad8(n):
    return -(-n // 8) * 8


def doubled(s):
    return jnp.where(s > 0, 2.0 * s, -1.0)


def has_neighbour(axis):
    i = lax.axis_index(axis)
    return i > 0, i < lax.axis_size(axis) - 1


def strength_kernel(seeds, ranks, flags, sz_low, sy_low, up, dn, e_out, r_out, top_row, rm):
    depth, rows, width = ranks.shape
    zlo, zhi = has_neighbour("gz")
    ylo, yhi = has_neighbour("gy")
    shape = (rows, width)
    row = lax.broadcasted_iota(jnp.int32, shape, 0)
    col = lax.broadcasted_iota(jnp.int32, shape, 1)
    x_in = col < width - 1
    y_in = (row < rows - 1) | yhi
    y_first = row == 0
    y_last = row == rows - 1

    def sx_of(z):
        return jnp.where(x_in, seeds[0, z], 0.0)

    def sy_of(z):
        return jnp.where(y_in, seeds[1, z], 0.0)

    def sz_of(z):
        if z < 0:
            return jnp.where(zlo, sz_low[...], 0.0)
        s = seeds[2, z]
        return jnp.where(zhi, s, 0.0) if z == depth - 1 else s

    for z in range(depth):
        sx, sy, sz = sx_of(z), sy_of(z), sz_of(z)
        below = jnp.where(ylo, sy_low[pl.ds(z, 1), :], 0.0)
        sy_prev = jnp.where(y_first, below, pltpu.roll(sy, 1, 0))
        r = jnp.maximum(jnp.maximum(sx, pltpu.roll(sx, 1, 1)), jnp.maximum(sy, sy_prev))
        rm[z] = jnp.maximum(r, jnp.maximum(sz, sz_of(z - 1)))
    for z in range(depth):
        r = rm[z]
        tx, ty, tz = doubled(sx_of(z)), doubled(sy_of(z)), doubled(sz_of(z))
        e = jnp.where(tx >= r, 1, 0) + jnp.where(tx >= pltpu.roll(r, width - 1, 1), 2, 0)
        e += jnp.where(ty >= r, 4, 0)
        e += jnp.where((ty >= pltpu.roll(r, rows - 1, 0)) & ~y_last, 8, 0)
        e += jnp.where(tz >= r, 16, 0)
        if z < depth - 1:
            e += jnp.where(tz >= rm[z + 1], 32, 0)
        f = flags[z]
        p = jnp.where(f == 0, ranks[z], jnp.where(f == 2, -2.0, -1.0))
        ef = e.astype(jnp.float32)
        e_out[z] = e
        r_out[z] = p
        top_row[pl.ds(z, 1), :] = r[0:1]
        sl = sy_of(z)[rows - 1 : rows]
        k = depth - z
        if k <= H + 1:
            up[pl.ds((k - 1) * rows, rows), :] = ef
        base = (H + 1) * rows
        if k <= H:
            up[pl.ds(base + (k - 1) * rows, rows), :] = p
            up[pl.ds(base + H * rows + k - 1, 1), :] = sl
            up[pl.ds(base + H * rows + H + k - 1, 1), :] = r[0:1]
        if z == 0:
            dn[pl.ds(H * rows, rows), :] = r
        if z < H:
            dn[pl.ds(z * rows, rows), :] = ef
            dn[pl.ds(base + z * rows, rows), :] = p
            dn[pl.ds(base + H * rows + z, 1), :] = sl
            dn[pl.ds(base + H * rows + H + z, 1), :] = r[0:1]


def planes_kernel(zb, za, e_own, p_own, top_row, sz_low, sz_top, sy_last, dn_own, yup, ydn, e_ext, p_ext, strips):
    depth, rows, width = p_own.shape
    zlo, zhi = has_neighbour("gz")
    _, yhi = has_neighbour("gy")
    planes = depth + 2 * H
    base = (H + 1) * rows
    tail = base + H * rows
    half = rows - T

    def put(z, e, p):
        i = z + H
        e_ext[i + 1] = e
        ef = e.astype(jnp.float32)
        yup[pl.ds(i * T, T), :] = ef[half:]
        ydn[pl.ds(i * T, T), :] = ef[:T]
        p_ext[i] = p
        yup[pl.ds((planes + i) * T, T), :] = p[half:]
        ydn[pl.ds((planes + i) * T, T), :] = p[:T]

    def strip(z, s, r):
        i = z + H
        s = jnp.where(yhi, s, 0.0)
        strips[pl.ds(i, 1), :] = s
        strips[pl.ds(pad8(planes) + i, 1), :] = r
        yup[pl.ds(2 * planes * T + i, 1), :] = s
        ydn[pl.ds(2 * planes * T + i, 1), :] = r

    def from_below(k):
        e = jnp.where(zlo, zb[pl.ds((k - 1) * rows, rows), :], 0.0).astype(jnp.int32)
        if k == 1:
            r0 = dn_own[pl.ds(H * rows, rows), :]
            e = e + jnp.where((doubled(sz_low[...]) >= r0) & zlo, 32, 0)
        return e

    e_ext[0] = from_below(H + 1)
    for k in range(H, 0, -1):
        put(-k, from_below(k), zb[pl.ds(base + (k - 1) * rows, rows), :])
        strip(-k, zb[pl.ds(tail + k - 1, 1), :], zb[pl.ds(tail + H + k - 1, 1), :])
    for z in range(depth):
        e = e_own[z]
        if z == depth - 1:
            e = e + jnp.where((doubled(sz_top[...]) >= za[pl.ds(H * rows, rows), :]) & zhi, 32, 0)
        put(z, e, p_own[z])
        strip(z, sy_last[pl.ds(z, 1), :], top_row[pl.ds(z, 1), :])
    for k in range(H):
        put(depth + k, za[pl.ds(k * rows, rows), :].astype(jnp.int32), za[pl.ds(base + k * rows, rows), :])
        strip(depth + k, za[pl.ds(tail + k, 1), :], za[pl.ds(tail + H + k, 1), :])


def rounds_kernel(yb, ya, e_ext, p_ext, strips, state_out, count_out, es, ps, ns, bs, caps):
    depth, rows, width = state_out.shape
    planes = depth + 2 * H
    ylo, _ = has_neighbour("gy")
    own = 2 * T
    chunks = range(T, own + rows + T, T)
    shape = (T, width)
    row = lax.broadcasted_iota(jnp.int32, shape, 0)

    es[0, pl.ds(own, rows), :] = e_ext[0]

    @pl.loop(0, planes)
    def _(i):
        at = pl.multiple_of(i * T, T)
        eb = jnp.where(ylo, yb[pl.ds(at, T), :], 0.0).astype(jnp.int32)
        sb = yb[pl.ds(2 * planes * T + i, 1), :]
        r0 = strips[pl.ds(pad8(planes) + i, 1), :]
        feeds = jnp.where((doubled(sb) >= r0) & ylo, 8, 0)
        es[i + 1, pl.ds(T, T), :] = eb + jnp.where(row == T - 1, feeds, 0)
        e = e_ext[i + 1]
        s15 = strips[pl.ds(i, 1), :]
        feeds = jnp.where(doubled(s15) >= ya[pl.ds(2 * planes * T + i, 1), :], 8, 0)
        es[i + 1, pl.ds(own, rows - T), :] = e[: rows - T]
        es[i + 1, pl.ds(own + rows - T, T), :] = e[rows - T :] + jnp.where(row == T - 1, feeds, 0)
        es[i + 1, pl.ds(own + rows, T), :] = ya[pl.ds(at, T), :].astype(jnp.int32)
        at = pl.multiple_of((planes + i) * T, T)
        ps[i, pl.ds(T, T), :] = yb[pl.ds(at, T), :]
        ps[i, pl.ds(own, rows), :] = p_ext[i]
        ps[i, pl.ds(own + rows, T), :] = ya[pl.ds(at, T), :]

    @pl.loop(0, planes)
    def _(i):
        for c in chunks:
            here = pl.ds(c, T)
            e = es[i + 1, here, :]
            ex = pltpu.roll(e, 1, 1)
            ey = es[i + 1, pl.ds(c - 1, T), :]
            ez = es[i, here, :]
            bs[i, here, :] = (e & 21) | (ex & 2) | (ey & 8) | (ez & 32)
            infl = (e & 42) | (ex & 1) | (ey & 4) | (ez & 16)
            pairs = (infl & 21) + ((infl >> 1) & 21)
            many = (pairs & 3) + ((pairs >> 2) & 3) + (pairs >> 4)
            p = ps[i, here, :]
            ps[i, here, :] = jnp.where(p >= 0, p * (1 << many).astype(jnp.float32), p)
            for d, (v, m) in enumerate(((e, 3), (ex, 3), (e, 12), (ey, 12), (e, 48), (ez, 48))):
                caps[d, i, here, :] = jnp.where((v & m) != 0, BIG, -3.0)

    totals = []
    for step in range(ROUNDS):
        reach = H - 2 * step - 1
        last = step == ROUNDS - 1

        @pl.loop(H - reach, H + depth + reach)
        def _(i):
            for c in chunks:
                here = pl.ds(c, T)
                p = ps[i, here, :]
                near = jnp.minimum(pltpu.roll(p, width - 1, 1), caps[0, i, here, :])
                near = jnp.maximum(near, jnp.minimum(pltpu.roll(p, 1, 1), caps[1, i, here, :]))
                near = jnp.maximum(near, jnp.minimum(ps[i, pl.ds(c + 1, T), :], caps[2, i, here, :]))
                near = jnp.maximum(near, jnp.minimum(ps[i, pl.ds(c - 1, T), :], caps[3, i, here, :]))
                near = jnp.maximum(near, jnp.minimum(ps[i + 1, here, :], caps[4, i, here, :]))
                near = jnp.maximum(near, jnp.minimum(ps[i - 1, here, :], caps[5, i, here, :]))
                ns[i, here, :] = jnp.where((p >= 0) & (p > near), 63, 0)

        def hits(i, c):
            here = pl.ds(c, T)
            n = ns[i, here, :]
            hit = (pltpu.roll(n, width - 1, 1) & 1) | (pltpu.roll(n, 1, 1) & 2)
            hit |= (ns[i, pl.ds(c + 1, T), :] & 4) | (ns[i, pl.ds(c - 1, T), :] & 8)
            hit |= (ns[i + 1, here, :] & 16) | (ns[i - 1, here, :] & 32)
            return n != 0, (hit & bs[i, here, :]) != 0, ps[i, here, :]

        reach -= 1
        zero = jnp.zeros(shape, jnp.int32)
        if last:

            def body(z, total):
                for j in range(0, rows, T):
                    new, hit, p = hits(z + H, own + j)
                    old = jnp.where(p >= 0, jnp.where(hit, 1, 0), jnp.where(p == -2.0, 2, 1))
                    state = jnp.where(new, 2, old)
                    state_out[z, pl.ds(j, T), :] = state
                    total = total + jnp.where(state == 0, 1, 0)
                return total

            total = lax.fori_loop(0, depth, body, zero)
        else:

            def body(i, total):
                mine = ((i >= H) & (i < H + depth)).astype(jnp.int32)
                for c in chunks:
                    new, hit, p = hits(i, c)
                    p = jnp.where(new, -2.0, jnp.where((p >= 0) & hit, -1.0, p))
                    ps[i, pl.ds(c, T), :] = p
                    if own <= c < own + rows:
                        total = total + jnp.where(p >= 0, mine, 0)
                return total

            total = lax.fori_loop(H - reach, H + depth + reach, body, zero)
        totals.append(jnp.sum(total))
    lane = lax.broadcasted_iota(jnp.int32, count_out.shape, 2)
    count_out[...] = jnp.where(lane == 0, totals[0], jnp.where(lane == 1, totals[1], jnp.where(lane == 2, totals[2], 0)))


def shift(value, axis, step):
    count = lax.axis_size(axis)
    return lax.ppermute(value, axis, [(i, (i + step) % count) for i in range(count)])


def call(kernel, outs, scratch, limit, args):
    return pl.pallas_call(
        kernel,
        out_shape=outs,
        in_specs=[whole()] * len(args),
        out_specs=[whole()] * len(outs),
        scratch_shapes=scratch,
        compiler_params=pltpu.CompilerParams(vmem_limit_bytes=limit * 2**20),
    )(*args)


def per_device(ranks, seeds, flags):
    depth, rows, width = ranks.shape
    assert depth > H and rows >= 2 * T and H < T
    planes = depth + 2 * H
    devices = lax.axis_size("gz") * lax.axis_size("gy")
    f32, i32 = jnp.float32, jnp.int32
    of = jax.ShapeDtypeStruct
    sz_top = seeds[2, depth - 1]
    sy_last = seeds[1, :, rows - 1]
    sz_low = shift(sz_top, "gz", 1)
    sy_low = shift(sy_last, "gy", 1)
    message = of((pad8((2 * H + 1) * rows + 2 * H), width), f32)
    up, dn, e_own, p_own, top_row = call(
        strength_kernel,
        [message, message, of(ranks.shape, i32), of(ranks.shape, f32), of((depth, width), f32)],
        [pltpu.VMEM(ranks.shape, f32)],
        12,
        (seeds, ranks, flags, sz_low, sy_low),
    )
    zb = shift(up, "gz", 1)
    za = shift(dn, "gz", -1)
    message = of((2 * planes * T + pad8(planes), width), f32)
    yup, ydn, e_ext, p_ext, strips = call(
        planes_kernel,
        [
            message,
            message,
            of((planes + 1, rows, width), i32),
            of((planes, rows, width), f32),
            of((2 * pad8(planes), width), f32),
        ],
        [],
        12,
        (zb, za, e_own, p_own, top_row, sz_low, sz_top, sy_last, dn),
    )
    yb = shift(yup, "gy", 1)
    ya = shift(ydn, "gy", -1)
    tall = rows + 4 * T
    state, counts = call(
        rounds_kernel,
        [of(ranks.shape, i32), of((devices, 1, 128), i32)],
        [
            pltpu.VMEM((planes + 1, tall, width), i32),
            pltpu.VMEM((planes, tall, width), f32),
            pltpu.VMEM((planes, tall, width), i32),
            pltpu.VMEM((planes, tall, width), i32),
            pltpu.VMEM((6, planes, tall, width), f32),
        ],
        30,
        (yb, ya, e_ext, p_ext, strips),
    )
    everyone = lax.all_to_all(counts, ("gz", "gy"), 0, 0, tiled=True)
    undecided = jnp.sum(everyone, axis=(0, 1))[:ROUNDS]
    return (state, undecided)


def solution(mesh):
    return jax.shard_map(
        per_device,
        mesh=mesh,
        in_specs=(P("gz", "gy", None), P(None, "gz", "gy", None), P("gz", "gy", None)),
        out_specs=(P("gz", "gy", None), P()),
        check_vma=False,
    )
```

```python
import jax
import jax.numpy as jnp
from jax import lax
from jax.experimental import pallas as pl
from jax.experimental.pallas import tpu as pltpu
from jax.sharding import PartitionSpec as P

ROUNDS = 3
H = 2 * ROUNDS
T = 8
L = 128
BIG = 3.0e38
F32, I32 = jnp.float32, jnp.int32
CAPS, STATE, PATTERN, NEW = 0, 6, 0, 0


def vmem():
    return pl.BlockSpec(memory_space=pltpu.VMEM)


def neighbours(axis):
    i = lax.axis_index(axis)
    return i > 0, i < lax.axis_size(axis) - 1


def doubled(s):
    return jnp.where(s > 0, 2.0 * s, -1.0)


def scaled(p, bit):
    return jnp.where((bit != 0) & (p >= 0), 2.0 * p, p)


def edge_kernel(seeds, sz_top, sy_last, twice, rm):
    depth, rows, width = rm.shape
    _, zhi = neighbours("gz")
    _, yhi = neighbours("gy")
    shape = (rows, width)
    row = lax.broadcasted_iota(I32, shape, 0)
    x_in = lax.broadcasted_iota(I32, shape, 1) < width - 1
    y_in = (row < rows - 1) | yhi
    sz_top[...] = seeds[2, depth - 1]
    sz_prev = None
    for z in range(depth):
        sy_last[pl.ds(z, 1), :] = seeds[1, z, pl.ds(rows - 1, 1), :]
        sx = jnp.where(x_in, seeds[0, z], 0.0)
        sy = jnp.where(y_in, seeds[1, z], 0.0)
        sz = seeds[2, z]
        if z == depth - 1:
            sz = jnp.where(zhi, sz, 0.0)
        r = jnp.maximum(jnp.maximum(sx, pltpu.roll(sx, 1, 1)), jnp.maximum(sy, sz))
        r = jnp.maximum(r, jnp.where(row == 0, 0.0, pltpu.roll(sy, 1, 0)))
        rm[z] = r if z == 0 else jnp.maximum(r, sz_prev)
        sz_prev = sz
        for d, s in enumerate((sx, sy, sz)):
            twice[d, z] = doubled(s)


def packed_kernel(ranks, flags, packed):
    f = flags[...]
    packed[...] = jnp.where(f == 0, ranks[...], jnp.where(f == 2, -2.0, -1.0))


def strength_kernel(twice, rm, packed, sz_low, sy_low, up, dn, d_out, m_out):
    depth, rows, width = packed.shape
    zlo, _ = neighbours("gz")
    ylo, _ = neighbours("gy")
    row = lax.broadcasted_iota(I32, (rows, width), 0)
    tz_prev = doubled(jnp.where(zlo, sz_low[...], 0.0))
    for z in range(depth):
        sy_prev = jnp.where(ylo, sy_low[pl.ds(z, 1), :], 0.0)
        r = jnp.maximum(rm[z], jnp.where(row == 0, sy_prev, 0.0))
        if z == 0:
            r = jnp.maximum(r, jnp.where(zlo, sz_low[...], 0.0))
        tx, ty, tz = twice[0, z], twice[1, z], twice[2, z]
        ty_prev = jnp.where(row == 0, doubled(sy_prev), pltpu.roll(ty, 1, 0))
        d = jnp.where(tx >= r, 1, 0) + jnp.where(pltpu.roll(tx, 1, 1) >= r, 2, 0)
        d += jnp.where(ty >= r, 4, 0) + jnp.where(ty_prev >= r, 8, 0)
        d += jnp.where(tz >= r, 16, 0) + jnp.where(tz_prev >= r, 32, 0)
        d_out[z] = d
        tz_prev = tz
    for z in range(depth):
        d = d_out[z]
        i = (pltpu.roll(d, width - 1, 1) & 2) | (pltpu.roll(d, 1, 1) & 1)
        i |= jnp.where(row == rows - 1, 0, pltpu.roll(d, rows - 1, 0) & 8)
        i |= jnp.where(row == 0, 0, pltpu.roll(d, 1, 0) & 4)
        if z < depth - 1:
            i |= d_out[z + 1] & 32
        if z > 0:
            i |= d_out[z - 1] & 16
        pairs = (i & 21) + ((i >> 1) & 21)
        many = (pairs & 3) + ((pairs >> 2) & 3) + (pairs >> 4)
        p = packed[z]
        m = jnp.where(p >= 0, p * (1 << many).astype(F32), p)
        m_out[z] = m
        k = depth - z
        if k <= H:
            up[pl.ds((k - 1) * rows, rows), :] = d.astype(F32)
            up[pl.ds((H + k - 1) * rows, rows), :] = m
        if z < H:
            dn[pl.ds(z * rows, rows), :] = d.astype(F32)
            dn[pl.ds((H + z) * rows, rows), :] = m


def y_layout(depth):
    patterns, measures, at = [], [], 0
    for out, least in ((patterns, 1), (measures, 0)):
        for z in range(-H, depth + H):
            k = max(-z, z - depth + 1, 0)
            n = max(H - k, least)
            if n:
                out.append((z, n, at))
                at += n
    return patterns, measures, -(-at // T) * T


def planes_kernel(zb, za, d_own, m_own, ye, yo, d_ext, m_ext):
    depth, rows, _ = m_own.shape
    zlo, zhi = neighbours("gz")
    even = lax.axis_index("gy") % 2 == 0
    for k in range(1, H + 1):
        at, am = pl.ds((k - 1) * rows, rows), pl.ds((H + k - 1) * rows, rows)
        d_ext[H - k] = jnp.where(zlo, zb[at, :], 0.0).astype(I32)
        d_ext[H + depth + k - 1] = jnp.where(zhi, za[at, :], 0.0).astype(I32)
        m_ext[H - k] = zb[am, :]
        m_ext[H + depth + k - 1] = za[am, :]
    for z in range(depth):
        d_ext[H + z] = d_own[z]
        m_ext[H + z] = m_own[z]
    first, last = H, H + depth - 1
    m_ext[first - 1] = scaled(m_ext[first - 1], d_ext[first] & 32)
    m_ext[first] = scaled(m_ext[first], d_ext[first - 1] & 16)
    m_ext[last] = scaled(m_ext[last], d_ext[last + 1] & 32)
    m_ext[last + 1] = scaled(m_ext[last + 1], d_ext[last] & 16)
    patterns, measures, _ = y_layout(depth)

    def send(upward, downward):
        for z, n, at in patterns:
            e = d_ext[z + H].astype(F32)
            upward[pl.ds(at, n), :] = e[rows - n :]
            downward[pl.ds(at, n), :] = e[:n]
        for z, n, at in measures:
            e = m_ext[z + H]
            upward[pl.ds(at, n), :] = e[rows - n :]
            downward[pl.ds(at, n), :] = e[:n]

    @pl.when(even)
    def _():
        send(ye, yo)

    @pl.when(jnp.logical_not(even))
    def _():
        send(yo, ye)


def blocks(v):
    return jnp.stack([v[:, j : j + L] for j in range(0, v.shape[1], L)])


def x_next(v):
    r = pltpu.roll(v, L - 1, 2)
    lane = lax.broadcasted_iota(I32, v.shape, 2)
    return jnp.where(lane == L - 1, jnp.concatenate([r[1:], r[:1]], 0), r)


def x_prev(v):
    r = pltpu.roll(v, 1, 2)
    lane = lax.broadcasted_iota(I32, v.shape, 2)
    return jnp.where(lane == 0, jnp.concatenate([r[-1:], r[:-1]], 0), r)


def set_caps(fw, iw, i, at, n):
    def d_at(plane, row):
        return iw[PATTERN, plane, :, pl.ds(row, n), :]

    d = d_at(i, at)
    others = (x_next(d), x_prev(d), d_at(i, at + 1), d_at(i, at - 1), d_at(i + 1, at), d_at(i - 1, at))
    for j, other in enumerate(others):
        linked = (d & (1 << j)) | (other & (1 << (j ^ 1)))
        fw[CAPS + j, i, :, pl.ds(at, n), :] = jnp.where(linked != 0, BIG, -3.0)


def select(fw, iw, step, i, at, n):
    def cap(j):
        return fw[CAPS + j, i, :, pl.ds(at, n), :]

    def p_at(plane, row):
        return fw[STATE + step, plane, :, pl.ds(row, n), :]

    p = p_at(i, at)
    near = jnp.maximum(jnp.minimum(x_next(p), cap(0)), jnp.minimum(x_prev(p), cap(1)))
    near = jnp.maximum(near, jnp.minimum(p_at(i, at + 1), cap(2)))
    near = jnp.maximum(near, jnp.minimum(p_at(i, at - 1), cap(3)))
    near = jnp.maximum(near, jnp.minimum(p_at(i + 1, at), cap(4)))
    near = jnp.maximum(near, jnp.minimum(p_at(i - 1, at), cap(5)))
    new = (p >= 0) & (p > near)
    iw[NEW + 1 + step, i, :, pl.ds(at, n), :] = jnp.where(new, 63, 0)


def hits(fw, iw, step, i, at, n):
    def n_at(plane, row):
        return iw[NEW + 1 + step, plane, :, pl.ds(row, n), :]

    new = n_at(i, at)
    hit = (x_next(new) & 1) | (x_prev(new) & 2)
    hit |= (n_at(i, at + 1) & 4) | (n_at(i, at - 1) & 8)
    hit |= (n_at(i + 1, at) & 16) | (n_at(i - 1, at) & 32)
    hit &= iw[PATTERN, i, :, pl.ds(at, n), :]
    return new != 0, hit != 0, fw[STATE + step, i, :, pl.ds(at, n), :]


def update(fw, iw, step, i, at, n):
    new, hit, p = hits(fw, iw, step, i, at, n)
    p = jnp.where(new, -2.0, jnp.where((p >= 0) & hit, -1.0, p))
    fw[STATE + step + 1, i, :, pl.ds(at, n), :] = p


def inner_kernel(d_ext, m_ext, fw, iw):
    planes, rows, _ = m_ext.shape
    depth = planes - 2 * H

    @pl.loop(0, planes)
    def _(i):
        iw[PATTERN, i, :, pl.ds(T, rows), :] = blocks(d_ext[i])
        fw[STATE, i, :, pl.ds(T, rows), :] = blocks(m_ext[i])

    for stage in range(2 * ROUNDS - 1):
        step, reach = stage // 2, H - 1 - stage

        @pl.loop(H - reach, H + depth + reach)
        def _(i):
            for at in range(T, T + rows, T):
                if stage == 0:
                    set_caps(fw, iw, i, at, T)
                if stage % 2 == 0:
                    select(fw, iw, step, i, at, T)
                else:
                    update(fw, iw, step, i, at, T)


def outer_kernel(re, ro, fw_in, iw_in, state_out, count_out, fw, iw):
    del fw_in, iw_in
    depth, rows, width = state_out.shape
    planes = depth + 2 * H
    ylo, yhi = neighbours("gy")
    even = lax.axis_index("gy") % 2 == 0
    patterns, measures, _ = y_layout(depth)
    for z, n, at in patterns:
        e, o = re[pl.ds(at, n), :], ro[pl.ds(at, n), :]
        above = jnp.where(yhi, jnp.where(even, e, o), 0.0).astype(I32)
        below = jnp.where(ylo, jnp.where(even, o, e), 0.0).astype(I32)
        iw[PATTERN, z + H, :, pl.ds(T - n, n), :] = blocks(below)
        iw[PATTERN, z + H, :, pl.ds(T + rows, n), :] = blocks(above)
    for z, n, at in measures:
        e, o = re[pl.ds(at, n), :], ro[pl.ds(at, n), :]
        fw[STATE, z + H, :, pl.ds(T - n, n), :] = blocks(jnp.where(even, o, e))
        fw[STATE, z + H, :, pl.ds(T + rows, n), :] = blocks(jnp.where(even, e, o))

    def low(stage):
        return T - H + stage

    def high(stage):
        return T + rows + H - T - stage

    shape = (width // L, T, L)
    row = lax.broadcasted_iota(I32, shape, 1)

    @pl.loop(0, planes)
    def _(i):
        for at, one, two in ((low(0), H - 1, H), (high(0), T - H - 1, T - H)):
            d_next = iw[PATTERN, i, :, pl.ds(at + 1, T), :]
            d_prev = iw[PATTERN, i, :, pl.ds(at - 1, T), :]
            bit = jnp.where(row == one, d_next & 8, jnp.where(row == two, d_prev & 4, 0))
            here = pl.ds(at, T)
            fw[STATE, i, :, here, :] = scaled(fw[STATE, i, :, here, :], bit)

    for stage in range(2 * ROUNDS - 1):
        step, reach = stage // 2, H - 1 - stage

        @pl.loop(H - reach, H + depth + reach)
        def _(i):
            for at in (low(stage), high(stage)):
                if stage == 0:
                    set_caps(fw, iw, i, at, T)
                if stage % 2 == 0:
                    select(fw, iw, step, i, at, T)
                else:
                    update(fw, iw, step, i, at, T)

    def finish(z, totals):
        totals = list(totals)
        for at in range(0, rows, T):
            new, hit, p = hits(fw, iw, ROUNDS - 1, z + H, T + at, T)
            old = jnp.where(p >= 0, jnp.where(hit, 1, 0), jnp.where(p == -2.0, 2, 1))
            state = jnp.where(new, 2, old)
            for j in range(width // L):
                state_out[z, pl.ds(at, T), pl.ds(j * L, L)] = state[j]
            totals[-1] = totals[-1] + jnp.where(state == 0, 1, 0)
            for step in range(ROUNDS - 1):
                p = fw[STATE + step + 1, z + H, :, pl.ds(T + at, T), :]
                totals[step] = totals[step] + jnp.where(p >= 0, 1, 0)
        return tuple(totals)

    totals = lax.fori_loop(0, depth, finish, (jnp.zeros(shape, I32),) * ROUNDS)
    lane = lax.broadcasted_iota(I32, count_out.shape, 2)
    counts = jnp.zeros(count_out.shape, I32)
    for step in range(ROUNDS):
        counts = jnp.where(lane == step, jnp.sum(totals[step]), counts)
    count_out[...] = counts


def shift(value, axis, step):
    count = lax.axis_size(axis)
    return lax.ppermute(value, axis, [(i, (i + step) % count) for i in range(count)])


def swap(value, axis, odd):
    count = lax.axis_size(axis)
    pairs = [(i, i) for i in range(count)]
    for i in range(odd, count - 1, 2):
        pairs[i], pairs[i + 1] = (i, i + 1), (i + 1, i)
    return lax.ppermute(value, axis, pairs)


def call(kernel, outs, args, limit, cost, **more):
    specs = more.pop("in_specs", [vmem()] * len(args))
    return pl.pallas_call(
        kernel,
        out_shape=outs,
        in_specs=specs,
        out_specs=[vmem()] * len(outs),
        compiler_params=pltpu.CompilerParams(vmem_limit_bytes=limit * 2**20),
        cost_estimate=pl.CostEstimate(flops=cost, bytes_accessed=cost, transcendentals=0),
        **more,
    )(*args)


def per_device(ranks, seeds, flags):
    depth, rows, width = ranks.shape
    assert depth >= H and rows >= 2 * T and T == H + 2 and width % L == 0
    planes = depth + 2 * H
    devices = lax.axis_size("gz") * lax.axis_size("gy")
    of = jax.ShapeDtypeStruct
    own = [of(ranks.shape, F32)]
    sz_top, sy_last, twice, rm = call(
        edge_kernel,
        [of((rows, width), F32), of((depth, width), F32), of(seeds.shape, F32)] + own,
        (seeds,),
        8,
        4000000,
    )
    sz_low = shift(sz_top, "gz", 1)
    sy_low = shift(sy_last, "gy", 1)
    (packed,) = call(packed_kernel, own, (ranks, flags), 8, 4000000)
    message = of((2 * H * rows, width), F32)
    up, dn, d_own, m_own = call(
        strength_kernel,
        [message, message, of(ranks.shape, I32)] + own,
        (twice, rm, packed, sz_low, sy_low),
        8,
        4000000,
    )
    zb = shift(up, "gz", 1)
    za = shift(dn, "gz", -1)
    message = of((y_layout(depth)[2], width), F32)
    ext = (planes, rows, width)
    ye, yo, d_ext, m_ext = call(
        planes_kernel, [message, message, of(ext, I32), of(ext, F32)], (zb, za, d_own, m_own), 8, 4000000
    )
    re = swap(ye, "gy", 0)
    ro = swap(yo, "gy", 1)
    cells = (planes, width // L, rows + 2 * T, L)
    works = [of((STATE + ROUNDS,) + cells, F32), of((NEW + 1 + ROUNDS,) + cells, I32)]
    fw, iw = call(inner_kernel, works, (d_ext, m_ext), 8, 20000000)
    state, counts, _, _ = call(
        outer_kernel,
        [of(ranks.shape, I32), of((devices, 1, L), I32)] + works,
        (re, ro, fw, iw),
        8,
        20000000,
        input_output_aliases={2: 2, 3: 3},
    )
    everyone = lax.all_to_all(counts, ("gz", "gy"), 0, 0, tiled=True)
    undecided = jnp.sum(everyone, axis=(0, 1))[:ROUNDS]
    return (state, undecided)


def solution(mesh):
    return jax.shard_map(
        per_device,
        mesh=mesh,
        in_specs=(P("gz", "gy", None), P(None, "gz", "gy", None), P("gz", "gy", None)),
        out_specs=(P("gz", "gy", None), P()),
        check_vma=False,
    )
```

```python
import jax
import jax.numpy as jnp
from jax import lax
from jax.experimental import pallas as pl
from jax.experimental.pallas import tpu as pltpu
from jax.sharding import PartitionSpec as P

ROUNDS = 3
H = 2 * ROUNDS
T = 8
L = 128
BIG = 3.0e38
F32, I32 = jnp.float32, jnp.int32
CAPS, STATE, PATTERN, NEW = 0, 6, 0, 0


def vmem():
    return pl.BlockSpec(memory_space=pltpu.VMEM)


def neighbours(axis):
    i = lax.axis_index(axis)
    return i > 0, i < lax.axis_size(axis) - 1


def doubled(s):
    return jnp.where(s > 0, 2.0 * s, -1.0)


def scaled(p, bit):
    return jnp.where((bit != 0) & (p >= 0), 2.0 * p, p)


def edge_kernel(seeds, sz_top, sy_last, twice, rm):
    depth, rows, width = rm.shape
    _, zhi = neighbours("gz")
    _, yhi = neighbours("gy")
    shape = (rows, width)
    row = lax.broadcasted_iota(I32, shape, 0)
    x_in = lax.broadcasted_iota(I32, shape, 1) < width - 1
    y_in = (row < rows - 1) | yhi
    sz_top[...] = seeds[2, depth - 1]
    sz_prev = None
    for z in range(depth):
        sy_last[pl.ds(z, 1), :] = seeds[1, z, pl.ds(rows - 1, 1), :]
        sx = jnp.where(x_in, seeds[0, z], 0.0)
        sy = jnp.where(y_in, seeds[1, z], 0.0)
        sz = seeds[2, z]
        if z == depth - 1:
            sz = jnp.where(zhi, sz, 0.0)
        r = jnp.maximum(jnp.maximum(sx, pltpu.roll(sx, 1, 1)), jnp.maximum(sy, sz))
        r = jnp.maximum(r, jnp.where(row == 0, 0.0, pltpu.roll(sy, 1, 0)))
        rm[z] = r if z == 0 else jnp.maximum(r, sz_prev)
        sz_prev = sz
        for d, s in enumerate((sx, sy, sz)):
            twice[d, z] = doubled(s)


def packed_kernel(ranks, flags, packed):
    f = flags[...]
    packed[...] = jnp.where(f == 0, ranks[...], jnp.where(f == 2, -2.0, -1.0))


def strength_kernel(twice, rm, packed, sz_low, sy_low, up, dn, d_out, m_out):
    depth, rows, width = packed.shape
    zlo, _ = neighbours("gz")
    ylo, _ = neighbours("gy")
    row = lax.broadcasted_iota(I32, (rows, width), 0)
    tz_prev = doubled(jnp.where(zlo, sz_low[...], 0.0))
    for z in range(depth):
        sy_prev = jnp.where(ylo, sy_low[pl.ds(z, 1), :], 0.0)
        r = jnp.maximum(rm[z], jnp.where(row == 0, sy_prev, 0.0))
        if z == 0:
            r = jnp.maximum(r, jnp.where(zlo, sz_low[...], 0.0))
        tx, ty, tz = twice[0, z], twice[1, z], twice[2, z]
        ty_prev = jnp.where(row == 0, doubled(sy_prev), pltpu.roll(ty, 1, 0))
        d = jnp.where(tx >= r, 1, 0) + jnp.where(pltpu.roll(tx, 1, 1) >= r, 2, 0)
        d += jnp.where(ty >= r, 4, 0) + jnp.where(ty_prev >= r, 8, 0)
        d += jnp.where(tz >= r, 16, 0) + jnp.where(tz_prev >= r, 32, 0)
        d_out[z] = d
        tz_prev = tz
    for z in range(depth):
        d = d_out[z]
        i = (pltpu.roll(d, width - 1, 1) & 2) | (pltpu.roll(d, 1, 1) & 1)
        i |= jnp.where(row == rows - 1, 0, pltpu.roll(d, rows - 1, 0) & 8)
        i |= jnp.where(row == 0, 0, pltpu.roll(d, 1, 0) & 4)
        if z < depth - 1:
            i |= d_out[z + 1] & 32
        if z > 0:
            i |= d_out[z - 1] & 16
        pairs = (i & 21) + ((i >> 1) & 21)
        many = (pairs & 3) + ((pairs >> 2) & 3) + (pairs >> 4)
        p = packed[z]
        m = jnp.where(p >= 0, p * (1 << many).astype(F32), p)
        m_out[z] = m
        k = depth - z
        if k <= H:
            up[pl.ds((k - 1) * rows, rows), :] = d.astype(F32)
            up[pl.ds((H + k - 1) * rows, rows), :] = m
        if z < H:
            dn[pl.ds(z * rows, rows), :] = d.astype(F32)
            dn[pl.ds((H + z) * rows, rows), :] = m


def y_layout(depth):
    patterns, measures, at = [], [], 0
    for out, least in ((patterns, 1), (measures, 0)):
        for z in range(-H, depth + H):
            k = max(-z, z - depth + 1, 0)
            n = max(H - k, least)
            if n:
                out.append((z, n, at))
                at += n
    return patterns, measures, -(-at // T) * T


def planes_kernel(zb, za, d_own, m_own, yo, ye, d_ext, m_ext):
    depth, rows, _ = m_own.shape
    zlo, zhi = neighbours("gz")
    even = lax.axis_index("gy") % 2 == 0
    for k in range(1, H + 1):
        at, am = pl.ds((k - 1) * rows, rows), pl.ds((H + k - 1) * rows, rows)
        d_ext[H - k] = jnp.where(zlo, zb[at, :], 0.0).astype(I32)
        d_ext[H + depth + k - 1] = jnp.where(zhi, za[at, :], 0.0).astype(I32)
        m_ext[H - k] = zb[am, :]
        m_ext[H + depth + k - 1] = za[am, :]
    for z in range(depth):
        d_ext[H + z] = d_own[z]
        m_ext[H + z] = m_own[z]
    first, last = H, H + depth - 1
    m_ext[first - 1] = scaled(m_ext[first - 1], d_ext[first] & 32)
    m_ext[first] = scaled(m_ext[first], d_ext[first - 1] & 16)
    m_ext[last] = scaled(m_ext[last], d_ext[last + 1] & 32)
    m_ext[last + 1] = scaled(m_ext[last + 1], d_ext[last] & 16)
    patterns, measures, _ = y_layout(depth)

    def send(upward, downward):
        for z, n, at in patterns:
            e = d_ext[z + H].astype(F32)
            upward[pl.ds(at, n), :] = e[rows - n :]
            downward[pl.ds(at, n), :] = e[:n]
        for z, n, at in measures:
            e = m_ext[z + H]
            upward[pl.ds(at, n), :] = e[rows - n :]
            downward[pl.ds(at, n), :] = e[:n]

    @pl.when(even)
    def _():
        send(ye, yo)

    @pl.when(jnp.logical_not(even))
    def _():
        send(yo, ye)


def blocks(v):
    return jnp.stack([v[:, j : j + L] for j in range(0, v.shape[1], L)])


def x_next(v):
    r = pltpu.roll(v, L - 1, 2)
    lane = lax.broadcasted_iota(I32, v.shape, 2)
    return jnp.where(lane == L - 1, jnp.concatenate([r[1:], r[:1]], 0), r)


def x_prev(v):
    r = pltpu.roll(v, 1, 2)
    lane = lax.broadcasted_iota(I32, v.shape, 2)
    return jnp.where(lane == 0, jnp.concatenate([r[-1:], r[:-1]], 0), r)


def set_caps(fw, iw, sites):
    found = []
    for i, at in sites:

        def d_at(plane, row):
            return iw[PATTERN, plane, :, pl.ds(row, T), :]

        d = d_at(i, at)
        others = (x_next(d), x_prev(d), d_at(i, at + 1), d_at(i, at - 1), d_at(i + 1, at), d_at(i - 1, at))
        found.append([(d & (1 << j)) | (other & (1 << (j ^ 1))) for j, other in enumerate(others)])
    caps = [[jnp.where(linked != 0, BIG, -3.0) for linked in some] for some in found]
    for (i, at), some in zip(sites, caps):
        for j, cap in enumerate(some):
            fw[CAPS + j, i, :, pl.ds(at, T), :] = cap
    return caps


def caps_of(fw, sites):
    return [[fw[CAPS + j, i, :, pl.ds(at, T), :] for j in range(6)] for i, at in sites]


def select(fw, iw, step, sites, caps):
    found = []
    for (i, at), cap in zip(sites, caps):

        def p_at(plane, row):
            return fw[STATE + step, plane, :, pl.ds(row, T), :]

        p = p_at(i, at)
        y = jnp.maximum(jnp.minimum(p_at(i, at + 1), cap[2]), jnp.minimum(p_at(i, at - 1), cap[3]))
        z = jnp.maximum(jnp.minimum(p_at(i + 1, at), cap[4]), jnp.minimum(p_at(i - 1, at), cap[5]))
        x = jnp.maximum(jnp.minimum(x_next(p), cap[0]), jnp.minimum(x_prev(p), cap[1]))
        found.append((p >= 0) & (p > jnp.maximum(jnp.maximum(y, z), x)))
    for (i, at), new in zip(sites, found):
        iw[NEW + 1 + step, i, :, pl.ds(at, T), :] = jnp.where(new, 63, 0)


def hits(fw, iw, step, i, at):
    def n_at(plane, row):
        return iw[NEW + 1 + step, plane, :, pl.ds(row, T), :]

    new = n_at(i, at)
    hit = ((n_at(i, at + 1) & 4) | (n_at(i, at - 1) & 8)) | ((n_at(i + 1, at) & 16) | (n_at(i - 1, at) & 32))
    hit |= (x_next(new) & 1) | (x_prev(new) & 2)
    hit &= iw[PATTERN, i, :, pl.ds(at, T), :]
    return new != 0, hit != 0, fw[STATE + step, i, :, pl.ds(at, T), :]


def update(fw, iw, step, sites):
    found = []
    for i, at in sites:
        new, hit, p = hits(fw, iw, step, i, at)
        found.append(jnp.where(new, -2.0, jnp.where((p >= 0) & hit, -1.0, p)))
    for (i, at), p in zip(sites, found):
        fw[STATE + step + 1, i, :, pl.ds(at, T), :] = p


def stages(fw, iw, depth, rows_of):
    for stage in range(2 * ROUNDS - 1):
        step, reach = stage // 2, H - 1 - stage
        each = max(n for n in (1, 2, 3, 4) if (depth + 2 * reach) % n == 0)

        @pl.loop(H - reach, H + depth + reach, step=each)
        def _(i):
            sites = [(i + j, at) for j in range(each) for at in rows_of(stage)]
            if stage == 0:
                select(fw, iw, step, sites, set_caps(fw, iw, sites))
            elif stage % 2 == 0:
                select(fw, iw, step, sites, caps_of(fw, sites))
            else:
                update(fw, iw, step, sites)


def inner_kernel(d_ext, m_ext, fw, iw):
    planes, rows, _ = m_ext.shape
    depth = planes - 2 * H

    @pl.loop(0, planes)
    def _(i):
        iw[PATTERN, i, :, pl.ds(T, rows), :] = blocks(d_ext[i])
        fw[STATE, i, :, pl.ds(T, rows), :] = blocks(m_ext[i])

    stages(fw, iw, depth, lambda stage: range(T, T + rows, T))


def outer_kernel(ro, re, fw_in, iw_in, state_out, count_out, fw, iw):
    del fw_in, iw_in
    depth, rows, width = state_out.shape
    planes = depth + 2 * H
    ylo, yhi = neighbours("gy")
    even = lax.axis_index("gy") % 2 == 0
    patterns, measures, _ = y_layout(depth)
    for z, n, at in patterns:
        e, o = re[pl.ds(at, n), :], ro[pl.ds(at, n), :]
        above = jnp.where(yhi, jnp.where(even, e, o), 0.0).astype(I32)
        below = jnp.where(ylo, jnp.where(even, o, e), 0.0).astype(I32)
        iw[PATTERN, z + H, :, pl.ds(T - n, n), :] = blocks(below)
        iw[PATTERN, z + H, :, pl.ds(T + rows, n), :] = blocks(above)
    for z, n, at in measures:
        e, o = re[pl.ds(at, n), :], ro[pl.ds(at, n), :]
        fw[STATE, z + H, :, pl.ds(T - n, n), :] = blocks(jnp.where(even, o, e))
        fw[STATE, z + H, :, pl.ds(T + rows, n), :] = blocks(jnp.where(even, e, o))

    def low(stage):
        return T - H + stage

    def high(stage):
        return T + rows + H - T - stage

    shape = (width // L, T, L)
    row = lax.broadcasted_iota(I32, shape, 1)

    @pl.loop(0, planes)
    def _(i):
        for at, one, two in ((low(0), H - 1, H), (high(0), T - H - 1, T - H)):
            d_next = iw[PATTERN, i, :, pl.ds(at + 1, T), :]
            d_prev = iw[PATTERN, i, :, pl.ds(at - 1, T), :]
            bit = jnp.where(row == one, d_next & 8, jnp.where(row == two, d_prev & 4, 0))
            here = pl.ds(at, T)
            fw[STATE, i, :, here, :] = scaled(fw[STATE, i, :, here, :], bit)

    stages(fw, iw, depth, lambda stage: (low(stage), high(stage)))

    def finish(z, totals):
        totals = list(totals)
        for at in range(0, rows, T):
            new, hit, p = hits(fw, iw, ROUNDS - 1, z + H, T + at)
            old = jnp.where(p >= 0, jnp.where(hit, 1, 0), jnp.where(p == -2.0, 2, 1))
            state = jnp.where(new, 2, old)
            for j in range(width // L):
                state_out[z, pl.ds(at, T), pl.ds(j * L, L)] = state[j]
            totals[-1] = totals[-1] + jnp.where(state == 0, 1, 0)
            for step in range(ROUNDS - 1):
                p = fw[STATE + step + 1, z + H, :, pl.ds(T + at, T), :]
                totals[step] = totals[step] + jnp.where(p >= 0, 1, 0)
        return tuple(totals)

    totals = lax.fori_loop(0, depth, finish, (jnp.zeros(shape, I32),) * ROUNDS)
    lane = lax.broadcasted_iota(I32, count_out.shape, 2)
    counts = jnp.zeros(count_out.shape, I32)
    for step in range(ROUNDS):
        counts = jnp.where(lane == step, jnp.sum(totals[step]), counts)
    count_out[...] = counts


def shift(value, axis, step):
    count = lax.axis_size(axis)
    return lax.ppermute(value, axis, [(i, (i + step) % count) for i in range(count)])


def swap(value, axis, odd):
    count = lax.axis_size(axis)
    pairs = [(i, i) for i in range(count)]
    for i in range(odd, count - 1, 2):
        pairs[i], pairs[i + 1] = (i, i + 1), (i + 1, i)
    return lax.ppermute(value, axis, pairs)


def call(kernel, outs, args, limit, cost, **more):
    specs = more.pop("in_specs", [vmem()] * len(args))
    return pl.pallas_call(
        kernel,
        out_shape=outs,
        in_specs=specs,
        out_specs=[vmem()] * len(outs),
        compiler_params=pltpu.CompilerParams(vmem_limit_bytes=limit * 2**20),
        cost_estimate=pl.CostEstimate(flops=cost, bytes_accessed=cost, transcendentals=0),
        **more,
    )(*args)


def per_device(ranks, seeds, flags):
    depth, rows, width = ranks.shape
    assert depth >= H and rows >= 2 * T and T == H + 2 and width % L == 0
    planes = depth + 2 * H
    devices = lax.axis_size("gz") * lax.axis_size("gy")
    of = jax.ShapeDtypeStruct
    own = [of(ranks.shape, F32)]
    sz_top, sy_last, twice, rm = call(
        edge_kernel,
        [of((rows, width), F32), of((depth, width), F32), of(seeds.shape, F32)] + own,
        (seeds,),
        8,
        4000000,
    )
    sz_low = shift(sz_top, "gz", 1)
    sy_low = shift(sy_last, "gy", 1)
    (packed,) = call(packed_kernel, own, (ranks, flags), 8, 4000000)
    message = of((2 * H * rows, width), F32)
    up, dn, d_own, m_own = call(
        strength_kernel,
        [message, message, of(ranks.shape, I32)] + own,
        (twice, rm, packed, sz_low, sy_low),
        8,
        4000000,
    )
    zb = shift(up, "gz", 1)
    za = shift(dn, "gz", -1)
    message = of((y_layout(depth)[2], width), F32)
    ext = (planes, rows, width)
    yo, ye, d_ext, m_ext = call(
        planes_kernel, [message, message, of(ext, I32), of(ext, F32)], (zb, za, d_own, m_own), 8, 4000000
    )
    ro = swap(yo, "gy", 1)
    re = swap(ye, "gy", 0)
    cells = (planes, width // L, rows + 2 * T, L)
    works = [of((STATE + ROUNDS,) + cells, F32), of((NEW + 1 + ROUNDS,) + cells, I32)]
    fw, iw = call(inner_kernel, works, (d_ext, m_ext), 8, 20000000)
    state, counts, _, _ = call(
        outer_kernel,
        [of(ranks.shape, I32), of((devices, 1, L), I32)] + works,
        (ro, re, fw, iw),
        8,
        20000000,
        input_output_aliases={2: 2, 3: 3},
    )
    everyone = lax.all_to_all(counts, ("gz", "gy"), 0, 0, tiled=True)
    undecided = jnp.sum(everyone, axis=(0, 1))[:ROUNDS]
    return (state, undecided)


def solution(mesh):
    return jax.shard_map(
        per_device,
        mesh=mesh,
        in_specs=(P("gz", "gy", None), P(None, "gz", "gy", None), P("gz", "gy", None)),
        out_specs=(P("gz", "gy", None), P()),
        check_vma=False,
    )
```

```python
import jax
import jax.numpy as jnp
from jax import lax
from jax.experimental import pallas as pl
from jax.experimental.pallas import tpu as pltpu
from jax.sharding import PartitionSpec as P

ROUNDS = 3
H = 2 * ROUNDS
T = 8
RELAYED = 2
L = 128
BIG = 3.0e38
F32, I32 = jnp.float32, jnp.int32
CAPS, STATE, PATTERN, NEW = 0, 6, 0, 0


def vmem():
    return pl.BlockSpec(memory_space=pltpu.VMEM)


def neighbours(axis):
    i = lax.axis_index(axis)
    return i > 0, i < lax.axis_size(axis) - 1


def doubled(s):
    return jnp.where(s > 0, 2.0 * s, -1.0)


def scaled(p, bit):
    return jnp.where((bit != 0) & (p >= 0), 2.0 * p, p)


def edge_kernel(seeds, sz_top, sy_last, twice, rm):
    depth, rows, width = rm.shape
    _, zhi = neighbours("gz")
    _, yhi = neighbours("gy")
    shape = (rows, width)
    row = lax.broadcasted_iota(I32, shape, 0)
    x_in = lax.broadcasted_iota(I32, shape, 1) < width - 1
    y_in = (row < rows - 1) | yhi
    sz_top[...] = seeds[2, depth - 1]
    sz_prev = None
    for z in range(depth):
        sy_last[pl.ds(z, 1), :] = seeds[1, z, pl.ds(rows - 1, 1), :]
        sx = jnp.where(x_in, seeds[0, z], 0.0)
        sy = jnp.where(y_in, seeds[1, z], 0.0)
        sz = seeds[2, z]
        if z == depth - 1:
            sz = jnp.where(zhi, sz, 0.0)
        r = jnp.maximum(jnp.maximum(sx, pltpu.roll(sx, 1, 1)), jnp.maximum(sy, sz))
        r = jnp.maximum(r, jnp.where(row == 0, 0.0, pltpu.roll(sy, 1, 0)))
        rm[z] = r if z == 0 else jnp.maximum(r, sz_prev)
        sz_prev = sz
        for d, s in enumerate((sx, sy, sz)):
            twice[d, z] = doubled(s)


def packed_kernel(ranks, flags, packed):
    f = flags[...]
    packed[...] = jnp.where(f == 0, ranks[...], jnp.where(f == 2, -2.0, -1.0))


def plane_lists(depth):
    both = list(range(H - RELAYED, H))
    partner = [z for z in range(depth - H, depth) if z not in both]
    other = list(range(H - RELAYED))
    return both, partner, other


def strength_kernel(twice, rm, packed, sz_low, sy_low, both, partner, other, d_out, m_out):
    depth, rows, width = packed.shape
    zlo, _ = neighbours("gz")
    ylo, _ = neighbours("gy")
    row = lax.broadcasted_iota(I32, (rows, width), 0)
    tz_prev = doubled(jnp.where(zlo, sz_low[...], 0.0))
    for z in range(depth):
        sy_prev = jnp.where(ylo, sy_low[pl.ds(z, 1), :], 0.0)
        r = jnp.maximum(rm[z], jnp.where(row == 0, sy_prev, 0.0))
        if z == 0:
            r = jnp.maximum(r, jnp.where(zlo, sz_low[...], 0.0))
        tx, ty, tz = twice[0, z], twice[1, z], twice[2, z]
        ty_prev = jnp.where(row == 0, doubled(sy_prev), pltpu.roll(ty, 1, 0))
        d = jnp.where(tx >= r, 1, 0) + jnp.where(pltpu.roll(tx, 1, 1) >= r, 2, 0)
        d += jnp.where(ty >= r, 4, 0) + jnp.where(ty_prev >= r, 8, 0)
        d += jnp.where(tz >= r, 16, 0) + jnp.where(tz_prev >= r, 32, 0)
        d_out[z] = d
        tz_prev = tz
    for z in range(depth):
        d = d_out[z]
        i = (pltpu.roll(d, width - 1, 1) & 2) | (pltpu.roll(d, 1, 1) & 1)
        i |= jnp.where(row == rows - 1, 0, pltpu.roll(d, rows - 1, 0) & 8)
        i |= jnp.where(row == 0, 0, pltpu.roll(d, 1, 0) & 4)
        if z < depth - 1:
            i |= d_out[z + 1] & 32
        if z > 0:
            i |= d_out[z - 1] & 16
        pairs = (i & 21) + ((i >> 1) & 21)
        many = (pairs & 3) + ((pairs >> 2) & 3) + (pairs >> 4)
        p = packed[z]
        m = jnp.where(p >= 0, p * (1 << many).astype(F32), p)
        m_out[z] = m
    even = lax.axis_index("gz") % 2 == 0

    def send(place):
        for ref, zs in zip((both, partner, other), plane_lists(depth)):
            for j, z in enumerate(zs):
                ref[pl.ds(j * rows, rows), :] = d_out[place(z)].astype(F32)
                ref[pl.ds((len(zs) + j) * rows, rows), :] = m_out[place(z)]

    @pl.when(even)
    def _():
        send(lambda z: z)

    @pl.when(jnp.logical_not(even))
    def _():
        send(lambda z: depth - 1 - z)


def y_layout(depth):
    patterns, measures, at = [], [], 0
    for out, least in ((patterns, 1), (measures, 0)):
        for z in range(-H, depth + H):
            k = max(-z, z - depth + 1, 0)
            n = max(H - k, least)
            if n:
                out.append((z, n, at))
                at += n
    return patterns, measures, -(-at // T) * T


def planes_kernel(both, partner, other, relayed, d_own, m_own, yo, ye, d_ext, m_ext):
    depth, rows, _ = m_own.shape
    zlo, zhi = neighbours("gz")
    above = lax.axis_index("gz") % 2 == 0
    even = lax.axis_index("gy") % 2 == 0

    def put(ref, zs, above, distance):
        for j, z in enumerate(zs):
            k = distance(z)
            i = jnp.where(above, H + depth + k - 1, H - k)
            d = ref[pl.ds(j * rows, rows), :]
            d_ext[i] = jnp.where((above & zhi) | (jnp.logical_not(above) & zlo), d, 0.0).astype(I32)
            m_ext[i] = ref[pl.ds((len(zs) + j) * rows, rows), :]

    for_both, for_partner, for_other = plane_lists(depth)
    put(both, for_both, above, lambda z: depth - z)
    put(partner, for_partner, above, lambda z: depth - z)
    put(other, for_other, jnp.logical_not(above), lambda z: z + 1)
    put(relayed, for_both, jnp.logical_not(above), lambda z: z + 1)
    for z in range(depth):
        d_ext[H + z] = d_own[z]
        m_ext[H + z] = m_own[z]
    first, last = H, H + depth - 1
    m_ext[first - 1] = scaled(m_ext[first - 1], d_ext[first] & 32)
    m_ext[first] = scaled(m_ext[first], d_ext[first - 1] & 16)
    m_ext[last] = scaled(m_ext[last], d_ext[last + 1] & 32)
    m_ext[last + 1] = scaled(m_ext[last + 1], d_ext[last] & 16)
    patterns, measures, _ = y_layout(depth)

    def send(upward, downward):
        for z, n, at in patterns:
            e = d_ext[z + H].astype(F32)
            upward[pl.ds(at, n), :] = e[rows - n :]
            downward[pl.ds(at, n), :] = e[:n]
        for z, n, at in measures:
            e = m_ext[z + H]
            upward[pl.ds(at, n), :] = e[rows - n :]
            downward[pl.ds(at, n), :] = e[:n]

    @pl.when(even)
    def _():
        send(ye, yo)

    @pl.when(jnp.logical_not(even))
    def _():
        send(yo, ye)


def blocks(v):
    return jnp.stack([v[:, j : j + L] for j in range(0, v.shape[1], L)])


def x_next(v):
    r = pltpu.roll(v, L - 1, 2)
    lane = lax.broadcasted_iota(I32, v.shape, 2)
    return jnp.where(lane == L - 1, jnp.concatenate([r[1:], r[:1]], 0), r)


def x_prev(v):
    r = pltpu.roll(v, 1, 2)
    lane = lax.broadcasted_iota(I32, v.shape, 2)
    return jnp.where(lane == 0, jnp.concatenate([r[-1:], r[:-1]], 0), r)


def set_caps(fw, iw, sites):
    found = []
    for i, at in sites:

        def d_at(plane, row):
            return iw[PATTERN, plane, :, pl.ds(row, T), :]

        d = d_at(i, at)
        others = (x_next(d), x_prev(d), d_at(i, at + 1), d_at(i, at - 1), d_at(i + 1, at), d_at(i - 1, at))
        found.append([(d & (1 << j)) | (other & (1 << (j ^ 1))) for j, other in enumerate(others)])
    caps = [[jnp.where(linked != 0, BIG, -3.0) for linked in some] for some in found]
    for (i, at), some in zip(sites, caps):
        for j, cap in enumerate(some):
            fw[CAPS + j, i, :, pl.ds(at, T), :] = cap
    return caps


def caps_of(fw, sites):
    return [[fw[CAPS + j, i, :, pl.ds(at, T), :] for j in range(6)] for i, at in sites]


def select(fw, iw, step, sites, caps):
    found = []
    for (i, at), cap in zip(sites, caps):

        def p_at(plane, row):
            return fw[STATE + step, plane, :, pl.ds(row, T), :]

        p = p_at(i, at)
        y = jnp.maximum(jnp.minimum(p_at(i, at + 1), cap[2]), jnp.minimum(p_at(i, at - 1), cap[3]))
        z = jnp.maximum(jnp.minimum(p_at(i + 1, at), cap[4]), jnp.minimum(p_at(i - 1, at), cap[5]))
        x = jnp.maximum(jnp.minimum(x_next(p), cap[0]), jnp.minimum(x_prev(p), cap[1]))
        found.append((p >= 0) & (p > jnp.maximum(jnp.maximum(y, z), x)))
    for (i, at), new in zip(sites, found):
        iw[NEW + 1 + step, i, :, pl.ds(at, T), :] = jnp.where(new, 63, 0)


def hits(fw, iw, step, i, at):
    def n_at(plane, row):
        return iw[NEW + 1 + step, plane, :, pl.ds(row, T), :]

    new = n_at(i, at)
    hit = ((n_at(i, at + 1) & 4) | (n_at(i, at - 1) & 8)) | ((n_at(i + 1, at) & 16) | (n_at(i - 1, at) & 32))
    hit |= (x_next(new) & 1) | (x_prev(new) & 2)
    hit &= iw[PATTERN, i, :, pl.ds(at, T), :]
    return new != 0, hit != 0, fw[STATE + step, i, :, pl.ds(at, T), :]


def update(fw, iw, step, sites):
    found = []
    for i, at in sites:
        new, hit, p = hits(fw, iw, step, i, at)
        found.append(jnp.where(new, -2.0, jnp.where((p >= 0) & hit, -1.0, p)))
    for (i, at), p in zip(sites, found):
        fw[STATE + step + 1, i, :, pl.ds(at, T), :] = p


def stages(fw, iw, depth, rows_of):
    for stage in range(2 * ROUNDS - 1):
        step, reach = stage // 2, H - 1 - stage
        each = max(n for n in (1, 2, 3, 4) if (depth + 2 * reach) % n == 0)

        @pl.loop(H - reach, H + depth + reach, step=each)
        def _(i):
            sites = [(i + j, at) for j in range(each) for at in rows_of(stage)]
            if stage == 0:
                select(fw, iw, step, sites, set_caps(fw, iw, sites))
            elif stage % 2 == 0:
                select(fw, iw, step, sites, caps_of(fw, sites))
            else:
                update(fw, iw, step, sites)


def inner_kernel(d_ext, m_ext, fw, iw):
    planes, rows, _ = m_ext.shape
    depth = planes - 2 * H

    @pl.loop(0, planes)
    def _(i):
        iw[PATTERN, i, :, pl.ds(T, rows), :] = blocks(d_ext[i])
        fw[STATE, i, :, pl.ds(T, rows), :] = blocks(m_ext[i])

    stages(fw, iw, depth, lambda stage: range(T, T + rows, T))


def outer_kernel(ro, re, fw_in, iw_in, state_out, count_out, fw, iw):
    del fw_in, iw_in
    depth, rows, width = state_out.shape
    planes = depth + 2 * H
    ylo, yhi = neighbours("gy")
    even = lax.axis_index("gy") % 2 == 0
    patterns, measures, _ = y_layout(depth)
    for z, n, at in patterns:
        e, o = re[pl.ds(at, n), :], ro[pl.ds(at, n), :]
        above = jnp.where(yhi, jnp.where(even, e, o), 0.0).astype(I32)
        below = jnp.where(ylo, jnp.where(even, o, e), 0.0).astype(I32)
        iw[PATTERN, z + H, :, pl.ds(T - n, n), :] = blocks(below)
        iw[PATTERN, z + H, :, pl.ds(T + rows, n), :] = blocks(above)
    for z, n, at in measures:
        e, o = re[pl.ds(at, n), :], ro[pl.ds(at, n), :]
        fw[STATE, z + H, :, pl.ds(T - n, n), :] = blocks(jnp.where(even, o, e))
        fw[STATE, z + H, :, pl.ds(T + rows, n), :] = blocks(jnp.where(even, e, o))

    def low(stage):
        return T - H + stage

    def high(stage):
        return T + rows + H - T - stage

    shape = (width // L, T, L)
    row = lax.broadcasted_iota(I32, shape, 1)

    @pl.loop(0, planes)
    def _(i):
        for at, one, two in ((low(0), H - 1, H), (high(0), T - H - 1, T - H)):
            d_next = iw[PATTERN, i, :, pl.ds(at + 1, T), :]
            d_prev = iw[PATTERN, i, :, pl.ds(at - 1, T), :]
            bit = jnp.where(row == one, d_next & 8, jnp.where(row == two, d_prev & 4, 0))
            here = pl.ds(at, T)
            fw[STATE, i, :, here, :] = scaled(fw[STATE, i, :, here, :], bit)

    stages(fw, iw, depth, lambda stage: (low(stage), high(stage)))

    def finish(z, totals):
        totals = list(totals)
        for at in range(0, rows, T):
            new, hit, p = hits(fw, iw, ROUNDS - 1, z + H, T + at)
            old = jnp.where(p >= 0, jnp.where(hit, 1, 0), jnp.where(p == -2.0, 2, 1))
            state = jnp.where(new, 2, old)
            for j in range(width // L):
                state_out[z, pl.ds(at, T), pl.ds(j * L, L)] = state[j]
            totals[-1] = totals[-1] + jnp.where(state == 0, 1, 0)
            for step in range(ROUNDS - 1):
                p = fw[STATE + step + 1, z + H, :, pl.ds(T + at, T), :]
                totals[step] = totals[step] + jnp.where(p >= 0, 1, 0)
        return tuple(totals)

    totals = lax.fori_loop(0, depth, finish, (jnp.zeros(shape, I32),) * ROUNDS)
    lane = lax.broadcasted_iota(I32, count_out.shape, 2)
    counts = jnp.zeros(count_out.shape, I32)
    for step in range(ROUNDS):
        counts = jnp.where(lane == step, jnp.sum(totals[step]), counts)
    count_out[...] = counts


def shift(value, axis, step):
    count = lax.axis_size(axis)
    return lax.ppermute(value, axis, [(i, (i + step) % count) for i in range(count)])


def swap(value, axis, odd):
    count = lax.axis_size(axis)
    pairs = [(i, i) for i in range(count)]
    for i in range(odd, count - 1, 2):
        pairs[i], pairs[i + 1] = (i, i + 1), (i + 1, i)
    return lax.ppermute(value, axis, pairs)


def relay(value, axis):
    last = lax.axis_size(axis) - 1
    pairs = [(i, min(i + 2, last) if i % 2 == 0 else max(i - 2, 0)) for i in range(last + 1)]
    return lax.ppermute(value, axis, pairs)


def call(kernel, outs, args, limit, cost, **more):
    specs = more.pop("in_specs", [vmem()] * len(args))
    return pl.pallas_call(
        kernel,
        out_shape=outs,
        in_specs=specs,
        out_specs=[vmem()] * len(outs),
        compiler_params=pltpu.CompilerParams(vmem_limit_bytes=limit * 2**20),
        cost_estimate=pl.CostEstimate(flops=cost, bytes_accessed=cost, transcendentals=0),
        **more,
    )(*args)


def per_device(ranks, seeds, flags):
    depth, rows, width = ranks.shape
    assert H + RELAYED <= depth + 1 <= 2 * H and lax.axis_size("gz") % 2 == 0 and rows >= 2 * T and T == H + 2 and width % L == 0
    planes = depth + 2 * H
    devices = lax.axis_size("gz") * lax.axis_size("gy")
    of = jax.ShapeDtypeStruct
    own = [of(ranks.shape, F32)]
    sz_top, sy_last, twice, rm = call(
        edge_kernel,
        [of((rows, width), F32), of((depth, width), F32), of(seeds.shape, F32)] + own,
        (seeds,),
        8,
        4000000,
    )
    sz_low = shift(sz_top, "gz", 1)
    sy_low = shift(sy_last, "gy", 1)
    (packed,) = call(packed_kernel, own, (ranks, flags), 8, 4000000)
    messages = [of((2 * len(zs) * rows, width), F32) for zs in plane_lists(depth)]
    both, partner, other, d_own, m_own = call(
        strength_kernel,
        messages + [of(ranks.shape, I32)] + own,
        (twice, rm, packed, sz_low, sy_low),
        8,
        4000000,
    )
    both = swap(both, "gz", 0)
    partner = swap(partner, "gz", 0)
    other, both = lax.optimization_barrier((other, both))
    relayed = relay(both, "gz")
    other = swap(other, "gz", 1)
    message = of((y_layout(depth)[2], width), F32)
    ext = (planes, rows, width)
    yo, ye, d_ext, m_ext = call(
        planes_kernel, [message, message, of(ext, I32), of(ext, F32)], (both, partner, other, relayed, d_own, m_own), 8, 4000000
    )
    ro = swap(yo, "gy", 1)
    re = swap(ye, "gy", 0)
    cells = (planes, width // L, rows + 2 * T, L)
    works = [of((STATE + ROUNDS,) + cells, F32), of((NEW + 1 + ROUNDS,) + cells, I32)]
    fw, iw = call(inner_kernel, works, (d_ext, m_ext), 8, 20000000)
    state, counts, _, _ = call(
        outer_kernel,
        [of(ranks.shape, I32), of((devices, 1, L), I32)] + works,
        (ro, re, fw, iw),
        8,
        20000000,
        input_output_aliases={2: 2, 3: 3},
    )
    everyone = lax.all_to_all(counts, ("gz", "gy"), 0, 0, tiled=True)
    undecided = jnp.sum(everyone, axis=(0, 1))[:ROUNDS]
    return (state, undecided)


def solution(mesh):
    return jax.shard_map(
        per_device,
        mesh=mesh,
        in_specs=(P("gz", "gy", None), P(None, "gz", "gy", None), P("gz", "gy", None)),
        out_specs=(P("gz", "gy", None), P()),
        check_vma=False,
    )
```

```python
import jax
import jax.numpy as jnp
from jax import lax
from jax.experimental import pallas as pl
from jax.experimental.pallas import tpu as pltpu
from jax.sharding import PartitionSpec as P


ROUNDS = 3
H = 2 * ROUNDS
T = 8
RELAYED = 2
L = 128
BIG = 3.0e38
F32, I32 = jnp.float32, jnp.int32
CAPS, STATE, PATTERN, NEW = 0, 6, 0, 0


def vmem():
    return pl.BlockSpec(memory_space=pltpu.VMEM)


def neighbours(axis):
    i = lax.axis_index(axis)
    return i > 0, i < lax.axis_size(axis) - 1


def doubled(s):
    return jnp.where(s > 0, 2.0 * s, -1.0)


def scaled(p, bit):
    return jnp.where((bit != 0) & (p >= 0), 2.0 * p, p)


def edge_kernel(seeds, sz_top, sy_last, twice, rm):
    depth, rows, width = rm.shape
    _, zhi = neighbours("gz")
    _, yhi = neighbours("gy")
    shape = (rows, width)
    row = lax.broadcasted_iota(I32, shape, 0)
    x_in = lax.broadcasted_iota(I32, shape, 1) < width - 1
    y_in = (row < rows - 1) | yhi
    sz_top[...] = seeds[2, depth - 1]
    sz_prev = None
    for z in range(depth):
        sy_last[pl.ds(z, 1), :] = seeds[1, z, pl.ds(rows - 1, 1), :]
        sx = jnp.where(x_in, seeds[0, z], 0.0)
        sy = jnp.where(y_in, seeds[1, z], 0.0)
        sz = seeds[2, z]
        if z == depth - 1:
            sz = jnp.where(zhi, sz, 0.0)
        r = jnp.maximum(jnp.maximum(sx, pltpu.roll(sx, 1, 1)), jnp.maximum(sy, sz))
        r = jnp.maximum(r, jnp.where(row == 0, 0.0, pltpu.roll(sy, 1, 0)))
        rm[z] = r if z == 0 else jnp.maximum(r, sz_prev)
        sz_prev = sz
        for d, s in enumerate((sx, sy, sz)):
            twice[d, z] = doubled(s)


def packed_kernel(ranks, flags, packed):
    f = flags[...]
    packed[...] = jnp.where(f == 0, ranks[...], jnp.where(f == 2, -2.0, -1.0))


def plane_lists(depth):
    both = list(range(H - RELAYED, H))
    partner = [z for z in range(depth - H, depth) if z not in both]
    other = list(range(H - RELAYED))
    return both, partner, other


def strength_kernel(twice, rm, packed, sz_low, sy_low, both, partner, other, d_out, m_out):
    depth, rows, width = packed.shape
    zlo, _ = neighbours("gz")
    ylo, _ = neighbours("gy")
    row = lax.broadcasted_iota(I32, (rows, width), 0)
    tz_prev = doubled(jnp.where(zlo, sz_low[...], 0.0))
    for z in range(depth):
        sy_prev = jnp.where(ylo, sy_low[pl.ds(z, 1), :], 0.0)
        r = jnp.maximum(rm[z], jnp.where(row == 0, sy_prev, 0.0))
        if z == 0:
            r = jnp.maximum(r, jnp.where(zlo, sz_low[...], 0.0))
        tx, ty, tz = twice[0, z], twice[1, z], twice[2, z]
        ty_prev = jnp.where(row == 0, doubled(sy_prev), pltpu.roll(ty, 1, 0))
        d = jnp.where(tx >= r, 1, 0) + jnp.where(pltpu.roll(tx, 1, 1) >= r, 2, 0)
        d += jnp.where(ty >= r, 4, 0) + jnp.where(ty_prev >= r, 8, 0)
        d += jnp.where(tz >= r, 16, 0) + jnp.where(tz_prev >= r, 32, 0)
        d_out[z] = d
        tz_prev = tz
    for z in range(depth):
        d = d_out[z]
        i = (pltpu.roll(d, width - 1, 1) & 2) | (pltpu.roll(d, 1, 1) & 1)
        i |= jnp.where(row == rows - 1, 0, pltpu.roll(d, rows - 1, 0) & 8)
        i |= jnp.where(row == 0, 0, pltpu.roll(d, 1, 0) & 4)
        if z < depth - 1:
            i |= d_out[z + 1] & 32
        if z > 0:
            i |= d_out[z - 1] & 16
        pairs = (i & 21) + ((i >> 1) & 21)
        many = (pairs & 3) + ((pairs >> 2) & 3) + (pairs >> 4)
        p = packed[z]
        m = jnp.where(p >= 0, p * (1 << many).astype(F32), p)
        m_out[z] = m
    even = lax.axis_index("gz") % 2 == 0

    def send(place):
        for ref, zs in zip((both, partner, other), plane_lists(depth)):
            for j, z in enumerate(zs):
                ref[pl.ds(j * rows, rows), :] = d_out[place(z)].astype(F32)
                ref[pl.ds((len(zs) + j) * rows, rows), :] = m_out[place(z)]

    @pl.when(even)
    def _():
        send(lambda z: z)

    @pl.when(jnp.logical_not(even))
    def _():
        send(lambda z: depth - 1 - z)


def y_layout(depth, early):
    patterns, measures, at = [], [], 0
    for out, least in ((patterns, 1), (measures, 0)):
        for z in range(-H, depth + H):
            k = max(-z, z - depth + 1, 0)
            n = max(H - k, least)
            ready = 0 <= z < depth and (least or 0 < z < depth - 1)
            if n and ready == early:
                out.append((z, n, at))
                at += n
    return patterns, measures, -(-at // T) * T


def send_rows(layout, pattern, measure, yo, ye):
    patterns, measures, _ = layout
    even = lax.axis_index("gy") % 2 == 0

    def send(upward, downward):
        for z, n, at in patterns:
            e = pattern(z).astype(F32)
            upward[pl.ds(at, n), :] = e[e.shape[0] - n :]
            downward[pl.ds(at, n), :] = e[:n]
        for z, n, at in measures:
            e = measure(z)
            upward[pl.ds(at, n), :] = e[e.shape[0] - n :]
            downward[pl.ds(at, n), :] = e[:n]

    @pl.when(even)
    def _():
        send(ye, yo)

    @pl.when(jnp.logical_not(even))
    def _():
        send(yo, ye)


def early_kernel(d_own, m_own, yo, ye):
    send_rows(y_layout(m_own.shape[0], True), lambda z: d_own[z], lambda z: m_own[z], yo, ye)


def planes_kernel(both, partner, other, relayed, d_own, m_own, yo, ye, d_ext, m_ext):
    depth, rows, _ = m_own.shape
    zlo, zhi = neighbours("gz")
    above = lax.axis_index("gz") % 2 == 0

    def put(ref, zs, above, distance):
        for j, z in enumerate(zs):
            k = distance(z)
            i = jnp.where(above, H + depth + k - 1, H - k)
            d = ref[pl.ds(j * rows, rows), :]
            d_ext[i] = jnp.where((above & zhi) | (jnp.logical_not(above) & zlo), d, 0.0).astype(I32)
            m_ext[i] = ref[pl.ds((len(zs) + j) * rows, rows), :]

    for_both, for_partner, for_other = plane_lists(depth)
    put(both, for_both, above, lambda z: depth - z)
    put(partner, for_partner, above, lambda z: depth - z)
    put(other, for_other, jnp.logical_not(above), lambda z: z + 1)
    put(relayed, for_both, jnp.logical_not(above), lambda z: z + 1)
    for z in range(depth):
        d_ext[H + z] = d_own[z]
        m_ext[H + z] = m_own[z]
    first, last = H, H + depth - 1
    m_ext[first - 1] = scaled(m_ext[first - 1], d_ext[first] & 32)
    m_ext[first] = scaled(m_ext[first], d_ext[first - 1] & 16)
    m_ext[last] = scaled(m_ext[last], d_ext[last + 1] & 32)
    m_ext[last + 1] = scaled(m_ext[last + 1], d_ext[last] & 16)
    send_rows(y_layout(depth, False), lambda z: d_ext[z + H], lambda z: m_ext[z + H], yo, ye)


def blocks(v):
    return jnp.stack([v[:, j : j + L] for j in range(0, v.shape[1], L)])


def x_next(v):
    r = pltpu.roll(v, L - 1, 2)
    lane = lax.broadcasted_iota(I32, v.shape, 2)
    return jnp.where(lane == L - 1, jnp.concatenate([r[1:], r[:1]], 0), r)


def x_prev(v):
    r = pltpu.roll(v, 1, 2)
    lane = lax.broadcasted_iota(I32, v.shape, 2)
    return jnp.where(lane == 0, jnp.concatenate([r[-1:], r[:-1]], 0), r)


def set_caps(fw, iw, sites):
    found = []
    for i, at in sites:

        def d_at(plane, row):
            return iw[PATTERN, plane, :, pl.ds(row, T), :]

        d = d_at(i, at)
        others = (x_next(d), x_prev(d), d_at(i, at + 1), d_at(i, at - 1), d_at(i + 1, at), d_at(i - 1, at))
        found.append([(d & (1 << j)) | (other & (1 << (j ^ 1))) for j, other in enumerate(others)])
    caps = [[jnp.where(linked != 0, BIG, -3.0) for linked in some] for some in found]
    for (i, at), some in zip(sites, caps):
        for j, cap in enumerate(some):
            fw[CAPS + j, i, :, pl.ds(at, T), :] = cap
    return caps


def caps_of(fw, sites):
    return [[fw[CAPS + j, i, :, pl.ds(at, T), :] for j in range(6)] for i, at in sites]


def select(fw, iw, step, sites, caps):
    found = []
    for (i, at), cap in zip(sites, caps):

        def p_at(plane, row):
            return fw[STATE + step, plane, :, pl.ds(row, T), :]

        p = p_at(i, at)
        y = jnp.maximum(jnp.minimum(p_at(i, at + 1), cap[2]), jnp.minimum(p_at(i, at - 1), cap[3]))
        z = jnp.maximum(jnp.minimum(p_at(i + 1, at), cap[4]), jnp.minimum(p_at(i - 1, at), cap[5]))
        x = jnp.maximum(jnp.minimum(x_next(p), cap[0]), jnp.minimum(x_prev(p), cap[1]))
        found.append((p >= 0) & (p > jnp.maximum(jnp.maximum(y, z), x)))
    for (i, at), new in zip(sites, found):
        iw[NEW + 1 + step, i, :, pl.ds(at, T), :] = jnp.where(new, 63, 0)


def hits(fw, iw, step, i, at):
    def n_at(plane, row):
        return iw[NEW + 1 + step, plane, :, pl.ds(row, T), :]

    new = n_at(i, at)
    hit = ((n_at(i, at + 1) & 4) | (n_at(i, at - 1) & 8)) | ((n_at(i + 1, at) & 16) | (n_at(i - 1, at) & 32))
    hit |= (x_next(new) & 1) | (x_prev(new) & 2)
    hit &= iw[PATTERN, i, :, pl.ds(at, T), :]
    return new != 0, hit != 0, fw[STATE + step, i, :, pl.ds(at, T), :]


def update(fw, iw, step, sites):
    found = []
    for i, at in sites:
        new, hit, p = hits(fw, iw, step, i, at)
        found.append(jnp.where(new, -2.0, jnp.where((p >= 0) & hit, -1.0, p)))
    for (i, at), p in zip(sites, found):
        fw[STATE + step + 1, i, :, pl.ds(at, T), :] = p


def stages(fw, iw, depth, rows_of):
    for stage in range(2 * ROUNDS - 1):
        step, reach = stage // 2, H - 1 - stage
        each = max(n for n in (1, 2, 3, 4) if (depth + 2 * reach) % n == 0)

        @pl.loop(H - reach, H + depth + reach, step=each)
        def _(i):
            sites = [(i + j, at) for j in range(each) for at in rows_of(stage)]
            if stage == 0:
                select(fw, iw, step, sites, set_caps(fw, iw, sites))
            elif stage % 2 == 0:
                select(fw, iw, step, sites, caps_of(fw, sites))
            else:
                update(fw, iw, step, sites)


def inner_kernel(d_ext, m_ext, fw, iw):
    planes, rows, _ = m_ext.shape
    depth = planes - 2 * H

    @pl.loop(0, planes)
    def _(i):
        iw[PATTERN, i, :, pl.ds(T, rows), :] = blocks(d_ext[i])
        fw[STATE, i, :, pl.ds(T, rows), :] = blocks(m_ext[i])

    stages(fw, iw, depth, lambda stage: range(T, T + rows, T))


def outer_kernel(ro1, re1, ro2, re2, fw_in, iw_in, state_out, count_out, fw, iw, state_ref, sems):
    del fw_in, iw_in
    depth, rows, width = state_ref.shape
    planes = depth + 2 * H
    ylo, yhi = neighbours("gy")
    even = lax.axis_index("gy") % 2 == 0
    for ro, re, early in ((ro1, re1, True), (ro2, re2, False)):
        patterns, measures, _ = y_layout(depth, early)
        for z, n, at in patterns:
            e, o = re[pl.ds(at, n), :], ro[pl.ds(at, n), :]
            above = jnp.where(yhi, jnp.where(even, e, o), 0.0).astype(I32)
            below = jnp.where(ylo, jnp.where(even, o, e), 0.0).astype(I32)
            iw[PATTERN, z + H, :, pl.ds(T - n, n), :] = blocks(below)
            iw[PATTERN, z + H, :, pl.ds(T + rows, n), :] = blocks(above)
        for z, n, at in measures:
            e, o = re[pl.ds(at, n), :], ro[pl.ds(at, n), :]
            fw[STATE, z + H, :, pl.ds(T - n, n), :] = blocks(jnp.where(even, o, e))
            fw[STATE, z + H, :, pl.ds(T + rows, n), :] = blocks(jnp.where(even, e, o))

    def low(stage):
        return T - H + stage

    def high(stage):
        return T + rows + H - T - stage

    shape = (width // L, T, L)
    row = lax.broadcasted_iota(I32, shape, 1)

    each = max(n for n in (1, 2, 4) if planes % n == 0)

    @pl.loop(0, planes, step=each)
    def _(i):
        sites = [(i + j, *edge) for j in range(each) for edge in ((low(0), H - 1, H), (high(0), T - H - 1, T - H))]
        found = []
        for i, at, one, two in sites:
            d_next = iw[PATTERN, i, :, pl.ds(at + 1, T), :]
            d_prev = iw[PATTERN, i, :, pl.ds(at - 1, T), :]
            bit = jnp.where(row == one, d_next & 8, jnp.where(row == two, d_prev & 4, 0))
            found.append(scaled(fw[STATE, i, :, pl.ds(at, T), :], bit))
        for (i, at, _, _), p in zip(sites, found):
            fw[STATE, i, :, pl.ds(at, T), :] = p

    stages(fw, iw, depth, lambda stage: (low(stage), high(stage)))

    def finish(z, totals):
        totals = list(totals)
        for at in range(0, rows, T):
            new, hit, p = hits(fw, iw, ROUNDS - 1, z + H, T + at)
            old = jnp.where(p >= 0, jnp.where(hit, 1, 0), jnp.where(p == -2.0, 2, 1))
            state = jnp.where(new, 2, old)
            for j in range(width // L):
                state_ref[z, pl.ds(at, T), pl.ds(j * L, L)] = state[j]
            totals[-1] = totals[-1] + jnp.where(state == 0, 1, 0)
            for step in range(ROUNDS - 1):
                p = fw[STATE + step + 1, z + H, :, pl.ds(T + at, T), :]
                totals[step] = totals[step] + jnp.where(p >= 0, 1, 0)
        pltpu.make_async_copy(state_ref.at[z], state_out.at[z], sems.at[z]).start()
        return tuple(totals)

    totals = lax.fori_loop(0, depth, finish, (jnp.zeros(shape, I32),) * ROUNDS)
    lane = lax.broadcasted_iota(I32, count_out.shape, 2)
    counts = jnp.zeros(count_out.shape, I32)
    for step in range(ROUNDS):
        counts = jnp.where(lane == step, jnp.sum(totals[step]), counts)
    count_out[...] = counts
    for z in range(depth):
        pltpu.make_async_copy(state_ref.at[z], state_out.at[z], sems.at[z]).wait()


def shift(value, axis, step):
    count = lax.axis_size(axis)
    return lax.ppermute(value, axis, [(i, (i + step) % count) for i in range(count)])


def swap(value, axis, odd):
    count = lax.axis_size(axis)
    pairs = [(i, i) for i in range(count)]
    for i in range(odd, count - 1, 2):
        pairs[i], pairs[i + 1] = (i, i + 1), (i + 1, i)
    return lax.ppermute(value, axis, pairs)


def relay(value, axis):
    last = lax.axis_size(axis) - 1
    pairs = [(i, min(i + 2, last) if i % 2 == 0 else max(i - 2, 0)) for i in range(last + 1)]
    return lax.ppermute(value, axis, pairs)


def call(kernel, outs, args, limit, cost, **more):
    return pl.pallas_call(
        kernel,
        out_shape=outs,
        in_specs=[vmem()] * len(args),
        out_specs=more.pop("out_specs", [vmem()] * len(outs)),
        compiler_params=pltpu.CompilerParams(vmem_limit_bytes=limit * 2**20),
        cost_estimate=pl.CostEstimate(flops=cost, bytes_accessed=cost, transcendentals=0),
        **more,
    )(*args)


def per_device(ranks, seeds, flags):
    depth, rows, width = ranks.shape
    assert H + RELAYED <= depth + 1 <= 2 * H and lax.axis_size("gz") % 2 == 0 and rows >= 2 * T and T == H + 2 and width % L == 0
    planes = depth + 2 * H
    devices = lax.axis_size("gz") * lax.axis_size("gy")
    of = jax.ShapeDtypeStruct
    own = [of(ranks.shape, F32)]
    sz_top, sy_last, twice, rm = call(
        edge_kernel,
        [of((rows, width), F32), of((depth, width), F32), of(seeds.shape, F32)] + own,
        (seeds,),
        8,
        4000000,
    )
    sz_low = shift(sz_top, "gz", 1)
    sy_low = shift(sy_last, "gy", 1)
    (packed,) = call(packed_kernel, own, (ranks, flags), 8, 4000000)
    messages = [of((2 * len(zs) * rows, width), F32) for zs in plane_lists(depth)]
    both, partner, other, d_own, m_own = call(
        strength_kernel,
        messages + [of(ranks.shape, I32)] + own,
        (twice, rm, packed, sz_low, sy_low),
        8,
        4000000,
    )
    both = swap(both, "gz", 0)
    partner = swap(partner, "gz", 0)
    other, both = lax.optimization_barrier((other, both))
    relayed = relay(both, "gz")
    other = swap(other, "gz", 1)
    message = of((y_layout(depth, True)[2], width), F32)
    yo, ye = call(early_kernel, [message, message], (d_own, m_own), 8, 1000000)
    ro1 = swap(yo, "gy", 1)
    re1 = swap(ye, "gy", 0)
    message = of((y_layout(depth, False)[2], width), F32)
    ext = (planes, rows, width)
    yo, ye, d_ext, m_ext = call(
        planes_kernel, [message, message, of(ext, I32), of(ext, F32)], (both, partner, other, relayed, d_own, m_own), 8, 4000000
    )
    ro2 = swap(yo, "gy", 1)
    re2 = swap(ye, "gy", 0)
    cells = (planes, width // L, rows + 2 * T, L)
    works = [of((STATE + ROUNDS,) + cells, F32), of((NEW + 1 + ROUNDS,) + cells, I32)]
    fw, iw = call(inner_kernel, works, (d_ext, m_ext), 8, 20000000)
    state, counts, _, _ = call(
        outer_kernel,
        [of(ranks.shape, I32), of((devices, 1, L), I32)] + works,
        (ro1, re1, ro2, re2, fw, iw),
        8,
        20000000,
        input_output_aliases={4: 2, 5: 3},
        out_specs=[pl.BlockSpec(memory_space=pl.ANY), vmem(), vmem(), vmem()],
        scratch_shapes=[pltpu.VMEM(ranks.shape, I32), pltpu.SemaphoreType.DMA((depth,))],
    )
    everyone = lax.all_to_all(counts, ("gz", "gy"), 0, 0, tiled=True)
    undecided = jnp.sum(everyone, axis=(0, 1))[:ROUNDS]
    return (state, undecided)


def solution(mesh):
    return jax.shard_map(
        per_device,
        mesh=mesh,
        in_specs=(P("gz", "gy", None), P(None, "gz", "gy", None), P("gz", "gy", None)),
        out_specs=(P("gz", "gy", None), P()),
        check_vma=False,
    )
```

```python
import jax
import jax.numpy as jnp
from jax import lax
from jax.experimental import pallas as pl
from jax.experimental.pallas import tpu as pltpu
from jax.sharding import PartitionSpec as P


ROUNDS = 3
H = 2 * ROUNDS
T = 8
RELAYED = 3
L = 128
BIG = 3.0e38
F32, I32 = jnp.float32, jnp.int32
CAPS, STATE, PATTERN, NEW = 0, 6, 0, 0


def vmem():
    return pl.BlockSpec(memory_space=pltpu.VMEM)


def neighbours(axis):
    i = lax.axis_index(axis)
    return i > 0, i < lax.axis_size(axis) - 1


def doubled(s):
    return jnp.where(s > 0, 2.0 * s, -1.0)


def scaled(p, bit):
    return jnp.where((bit != 0) & (p >= 0), 2.0 * p, p)


def edge_kernel(seeds, sz_top, sy_last, twice, rm):
    depth, rows, width = rm.shape
    _, zhi = neighbours("gz")
    _, yhi = neighbours("gy")
    shape = (rows, width)
    row = lax.broadcasted_iota(I32, shape, 0)
    x_in = lax.broadcasted_iota(I32, shape, 1) < width - 1
    y_in = (row < rows - 1) | yhi
    sz_top[...] = seeds[2, depth - 1]
    sz_prev = None
    for z in range(depth):
        sy_last[pl.ds(z, 1), :] = seeds[1, z, pl.ds(rows - 1, 1), :]
        sx = jnp.where(x_in, seeds[0, z], 0.0)
        sy = jnp.where(y_in, seeds[1, z], 0.0)
        sz = seeds[2, z]
        if z == depth - 1:
            sz = jnp.where(zhi, sz, 0.0)
        r = jnp.maximum(jnp.maximum(sx, pltpu.roll(sx, 1, 1)), jnp.maximum(sy, sz))
        r = jnp.maximum(r, jnp.where(row == 0, 0.0, pltpu.roll(sy, 1, 0)))
        rm[z] = r if z == 0 else jnp.maximum(r, sz_prev)
        sz_prev = sz
        for d, s in enumerate((sx, sy, sz)):
            twice[d, z] = doubled(s)


def packed_kernel(ranks, flags, packed):
    f = flags[...]
    packed[...] = jnp.where(f == 0, ranks[...], jnp.where(f == 2, -2.0, -1.0))


def plane_lists(depth):
    both = list(range(H - RELAYED, H))
    partner = [z for z in range(depth - H, depth) if z not in both]
    other = list(range(H - RELAYED))
    return both, partner, other


def strength_kernel(twice, rm, packed, sz_low, sy_low, both, partner, other, d_out, m_out):
    depth, rows, width = packed.shape
    zlo, _ = neighbours("gz")
    ylo, _ = neighbours("gy")
    row = lax.broadcasted_iota(I32, (rows, width), 0)
    tz_prev = doubled(jnp.where(zlo, sz_low[...], 0.0))
    for z in range(depth):
        sy_prev = jnp.where(ylo, sy_low[pl.ds(z, 1), :], 0.0)
        r = jnp.maximum(rm[z], jnp.where(row == 0, sy_prev, 0.0))
        if z == 0:
            r = jnp.maximum(r, jnp.where(zlo, sz_low[...], 0.0))
        tx, ty, tz = twice[0, z], twice[1, z], twice[2, z]
        ty_prev = jnp.where(row == 0, doubled(sy_prev), pltpu.roll(ty, 1, 0))
        d = jnp.where(tx >= r, 1, 0) + jnp.where(pltpu.roll(tx, 1, 1) >= r, 2, 0)
        d += jnp.where(ty >= r, 4, 0) + jnp.where(ty_prev >= r, 8, 0)
        d += jnp.where(tz >= r, 16, 0) + jnp.where(tz_prev >= r, 32, 0)
        d_out[z] = d
        tz_prev = tz
    for z in range(depth):
        d = d_out[z]
        i = (pltpu.roll(d, width - 1, 1) & 2) | (pltpu.roll(d, 1, 1) & 1)
        i |= jnp.where(row == rows - 1, 0, pltpu.roll(d, rows - 1, 0) & 8)
        i |= jnp.where(row == 0, 0, pltpu.roll(d, 1, 0) & 4)
        if z < depth - 1:
            i |= d_out[z + 1] & 32
        if z > 0:
            i |= d_out[z - 1] & 16
        pairs = (i & 21) + ((i >> 1) & 21)
        many = (pairs & 3) + ((pairs >> 2) & 3) + (pairs >> 4)
        p = packed[z]
        m = jnp.where(p >= 0, p * (1 << many).astype(F32), p)
        m_out[z] = m
    even = lax.axis_index("gz") % 2 == 0

    def send(place):
        for ref, zs in zip((both, partner, other), plane_lists(depth)):
            for j, z in enumerate(zs):
                ref[pl.ds(j * rows, rows), :] = d_out[place(z)].astype(F32)
                ref[pl.ds((len(zs) + j) * rows, rows), :] = m_out[place(z)]

    @pl.when(even)
    def _():
        send(lambda z: z)

    @pl.when(jnp.logical_not(even))
    def _():
        send(lambda z: depth - 1 - z)


def y_layout(depth, early):
    patterns, measures, at = [], [], 0
    for out, least in ((patterns, 1), (measures, 0)):
        for z in range(-H, depth + H):
            k = max(-z, z - depth + 1, 0)
            n = max(H - k, least)
            ready = 0 <= z < depth and (least or 0 < z < depth - 1)
            if n and ready == early:
                out.append((z, n, at))
                at += n
    return patterns, measures, -(-at // T) * T


def send_rows(layout, pattern, measure, yo, ye):
    patterns, measures, _ = layout
    even = lax.axis_index("gy") % 2 == 0

    def send(upward, downward):
        for z, n, at in patterns:
            e = pattern(z).astype(F32)
            upward[pl.ds(at, n), :] = e[e.shape[0] - n :]
            downward[pl.ds(at, n), :] = e[:n]
        for z, n, at in measures:
            e = measure(z)
            upward[pl.ds(at, n), :] = e[e.shape[0] - n :]
            downward[pl.ds(at, n), :] = e[:n]

    @pl.when(even)
    def _():
        send(ye, yo)

    @pl.when(jnp.logical_not(even))
    def _():
        send(yo, ye)


def early_kernel(d_own, m_own, yo, ye):
    send_rows(y_layout(m_own.shape[0], True), lambda z: d_own[z], lambda z: m_own[z], yo, ye)


def planes_kernel(both, partner, other, relayed, d_own, m_own, yo, ye, d_ext, m_ext):
    depth, rows, _ = m_own.shape
    zlo, zhi = neighbours("gz")
    above = lax.axis_index("gz") % 2 == 0

    def put(ref, zs, above, distance):
        for j, z in enumerate(zs):
            k = distance(z)
            i = jnp.where(above, H + depth + k - 1, H - k)
            d = ref[pl.ds(j * rows, rows), :]
            d_ext[i] = jnp.where((above & zhi) | (jnp.logical_not(above) & zlo), d, 0.0).astype(I32)
            m_ext[i] = ref[pl.ds((len(zs) + j) * rows, rows), :]

    for_both, for_partner, for_other = plane_lists(depth)
    put(both, for_both, above, lambda z: depth - z)
    put(partner, for_partner, above, lambda z: depth - z)
    put(other, for_other, jnp.logical_not(above), lambda z: z + 1)
    put(relayed, for_both, jnp.logical_not(above), lambda z: z + 1)
    for z in range(depth):
        d_ext[H + z] = d_own[z]
        m_ext[H + z] = m_own[z]
    first, last = H, H + depth - 1
    m_ext[first - 1] = scaled(m_ext[first - 1], d_ext[first] & 32)
    m_ext[first] = scaled(m_ext[first], d_ext[first - 1] & 16)
    m_ext[last] = scaled(m_ext[last], d_ext[last + 1] & 32)
    m_ext[last + 1] = scaled(m_ext[last + 1], d_ext[last] & 16)
    send_rows(y_layout(depth, False), lambda z: d_ext[z + H], lambda z: m_ext[z + H], yo, ye)


def blocks(v):
    return jnp.stack([v[:, j : j + L] for j in range(0, v.shape[1], L)])


def x_next(v):
    r = pltpu.roll(v, L - 1, 2)
    lane = lax.broadcasted_iota(I32, v.shape, 2)
    return jnp.where(lane == L - 1, jnp.concatenate([r[1:], r[:1]], 0), r)


def x_prev(v):
    r = pltpu.roll(v, 1, 2)
    lane = lax.broadcasted_iota(I32, v.shape, 2)
    return jnp.where(lane == 0, jnp.concatenate([r[-1:], r[:-1]], 0), r)


def set_caps(fw, iw, sites):
    found = []
    for i, at in sites:

        def d_at(plane, row):
            return iw[PATTERN, plane, :, pl.ds(row, T), :]

        d = d_at(i, at)
        others = (x_next(d), x_prev(d), d_at(i, at + 1), d_at(i, at - 1), d_at(i + 1, at), d_at(i - 1, at))
        found.append([(d & (1 << j)) | (other & (1 << (j ^ 1))) for j, other in enumerate(others)])
    caps = [[jnp.where(linked != 0, BIG, -3.0) for linked in some] for some in found]
    for (i, at), some in zip(sites, caps):
        for j, cap in enumerate(some):
            fw[CAPS + j, i, :, pl.ds(at, T), :] = cap
    return caps


def caps_of(fw, sites):
    return [[fw[CAPS + j, i, :, pl.ds(at, T), :] for j in range(6)] for i, at in sites]


def select(fw, iw, step, sites, caps):
    found = []
    for (i, at), cap in zip(sites, caps):

        def p_at(plane, row):
            return fw[STATE + step, plane, :, pl.ds(row, T), :]

        p = p_at(i, at)
        y = jnp.maximum(jnp.minimum(p_at(i, at + 1), cap[2]), jnp.minimum(p_at(i, at - 1), cap[3]))
        z = jnp.maximum(jnp.minimum(p_at(i + 1, at), cap[4]), jnp.minimum(p_at(i - 1, at), cap[5]))
        x = jnp.maximum(jnp.minimum(x_next(p), cap[0]), jnp.minimum(x_prev(p), cap[1]))
        found.append((p >= 0) & (p > jnp.maximum(jnp.maximum(y, z), x)))
    for (i, at), new in zip(sites, found):
        iw[NEW + 1 + step, i, :, pl.ds(at, T), :] = jnp.where(new, 63, 0)


def hits(fw, iw, step, i, at):
    def n_at(plane, row):
        return iw[NEW + 1 + step, plane, :, pl.ds(row, T), :]

    new = n_at(i, at)
    hit = ((n_at(i, at + 1) & 4) | (n_at(i, at - 1) & 8)) | ((n_at(i + 1, at) & 16) | (n_at(i - 1, at) & 32))
    hit |= (x_next(new) & 1) | (x_prev(new) & 2)
    hit &= iw[PATTERN, i, :, pl.ds(at, T), :]
    return new != 0, hit != 0, fw[STATE + step, i, :, pl.ds(at, T), :]


def update(fw, iw, step, sites):
    found = []
    for i, at in sites:
        new, hit, p = hits(fw, iw, step, i, at)
        found.append(jnp.where(new, -2.0, jnp.where((p >= 0) & hit, -1.0, p)))
    for (i, at), p in zip(sites, found):
        fw[STATE + step + 1, i, :, pl.ds(at, T), :] = p


def stages(fw, iw, depth, rows_of):
    for stage in range(2 * ROUNDS - 1):
        step, reach = stage // 2, H - 1 - stage
        each = max(n for n in (1, 2, 3, 4) if (depth + 2 * reach) % n == 0)

        @pl.loop(H - reach, H + depth + reach, step=each)
        def _(i):
            sites = [(i + j, at) for j in range(each) for at in rows_of(stage)]
            if stage == 0:
                select(fw, iw, step, sites, set_caps(fw, iw, sites))
            elif stage % 2 == 0:
                select(fw, iw, step, sites, caps_of(fw, sites))
            else:
                update(fw, iw, step, sites)


def inner_kernel(d_ext, m_ext, fw, iw):
    planes, rows, _ = m_ext.shape
    depth = planes - 2 * H

    @pl.loop(0, planes)
    def _(i):
        iw[PATTERN, i, :, pl.ds(T, rows), :] = blocks(d_ext[i])
        fw[STATE, i, :, pl.ds(T, rows), :] = blocks(m_ext[i])

    stages(fw, iw, depth, lambda stage: range(T, T + rows, T))


def outer_kernel(ro1, re1, ro2, re2, fw_in, iw_in, state_out, count_out, fw, iw, state_ref, sems):
    del fw_in, iw_in
    depth, rows, width = state_ref.shape
    planes = depth + 2 * H
    ylo, yhi = neighbours("gy")
    even = lax.axis_index("gy") % 2 == 0
    for ro, re, early in ((ro1, re1, True), (ro2, re2, False)):
        patterns, measures, _ = y_layout(depth, early)
        for z, n, at in patterns:
            e, o = re[pl.ds(at, n), :], ro[pl.ds(at, n), :]
            above = jnp.where(yhi, jnp.where(even, e, o), 0.0).astype(I32)
            below = jnp.where(ylo, jnp.where(even, o, e), 0.0).astype(I32)
            iw[PATTERN, z + H, :, pl.ds(T - n, n), :] = blocks(below)
            iw[PATTERN, z + H, :, pl.ds(T + rows, n), :] = blocks(above)
        for z, n, at in measures:
            e, o = re[pl.ds(at, n), :], ro[pl.ds(at, n), :]
            fw[STATE, z + H, :, pl.ds(T - n, n), :] = blocks(jnp.where(even, o, e))
            fw[STATE, z + H, :, pl.ds(T + rows, n), :] = blocks(jnp.where(even, e, o))

    def low(stage):
        return T - H + stage

    def high(stage):
        return T + rows + H - T - stage

    shape = (width // L, T, L)
    row = lax.broadcasted_iota(I32, shape, 1)

    each = max(n for n in (1, 2, 4) if planes % n == 0)

    @pl.loop(0, planes, step=each)
    def _(i):
        sites = [(i + j, *edge) for j in range(each) for edge in ((low(0), H - 1, H), (high(0), T - H - 1, T - H))]
        found = []
        for i, at, one, two in sites:
            d_next = iw[PATTERN, i, :, pl.ds(at + 1, T), :]
            d_prev = iw[PATTERN, i, :, pl.ds(at - 1, T), :]
            bit = jnp.where(row == one, d_next & 8, jnp.where(row == two, d_prev & 4, 0))
            found.append(scaled(fw[STATE, i, :, pl.ds(at, T), :], bit))
        for (i, at, _, _), p in zip(sites, found):
            fw[STATE, i, :, pl.ds(at, T), :] = p

    stages(fw, iw, depth, lambda stage: (low(stage), high(stage)))

    def finish(z, totals):
        totals = list(totals)
        for at in range(0, rows, T):
            new, hit, p = hits(fw, iw, ROUNDS - 1, z + H, T + at)
            old = jnp.where(p >= 0, jnp.where(hit, 1, 0), jnp.where(p == -2.0, 2, 1))
            state = jnp.where(new, 2, old)
            for j in range(width // L):
                state_ref[z, pl.ds(at, T), pl.ds(j * L, L)] = state[j]
            totals[-1] = totals[-1] + jnp.where(state == 0, 1, 0)
            for step in range(ROUNDS - 1):
                p = fw[STATE + step + 1, z + H, :, pl.ds(T + at, T), :]
                totals[step] = totals[step] + jnp.where(p >= 0, 1, 0)
        pltpu.make_async_copy(state_ref.at[z], state_out.at[z], sems.at[z]).start()
        return tuple(totals)

    totals = lax.fori_loop(0, depth, finish, (jnp.zeros(shape, I32),) * ROUNDS)
    lane = lax.broadcasted_iota(I32, count_out.shape, 2)
    counts = jnp.zeros(count_out.shape, I32)
    for step in range(ROUNDS):
        counts = jnp.where(lane == step, jnp.sum(totals[step]), counts)
    count_out[...] = counts
    for z in range(depth):
        pltpu.make_async_copy(state_ref.at[z], state_out.at[z], sems.at[z]).wait()


def shift(value, axis, step):
    count = lax.axis_size(axis)
    return lax.ppermute(value, axis, [(i, (i + step) % count) for i in range(count)])


def swap(value, axis, odd):
    count = lax.axis_size(axis)
    pairs = [(i, i) for i in range(count)]
    for i in range(odd, count - 1, 2):
        pairs[i], pairs[i + 1] = (i, i + 1), (i + 1, i)
    return lax.ppermute(value, axis, pairs)


def relay(value, axis):
    last = lax.axis_size(axis) - 1
    pairs = [(i, min(i + 2, last) if i % 2 == 0 else max(i - 2, 0)) for i in range(last + 1)]
    return lax.ppermute(value, axis, pairs)


def call(kernel, outs, args, limit, cost, **more):
    return pl.pallas_call(
        kernel,
        out_shape=outs,
        in_specs=[vmem()] * len(args),
        out_specs=more.pop("out_specs", [vmem()] * len(outs)),
        compiler_params=pltpu.CompilerParams(vmem_limit_bytes=limit * 2**20),
        cost_estimate=pl.CostEstimate(flops=cost, bytes_accessed=cost, transcendentals=0),
        **more,
    )(*args)


def per_device(ranks, seeds, flags):
    depth, rows, width = ranks.shape
    assert RELAYED <= 2 * H - depth and H < depth and lax.axis_size("gz") % 2 == 0 and rows >= 2 * T and T == H + 2 and width % L == 0
    planes = depth + 2 * H
    devices = lax.axis_size("gz") * lax.axis_size("gy")
    of = jax.ShapeDtypeStruct
    own = [of(ranks.shape, F32)]
    sz_top, sy_last, twice, rm = call(
        edge_kernel,
        [of((rows, width), F32), of((depth, width), F32), of(seeds.shape, F32)] + own,
        (seeds,),
        8,
        4000000,
    )
    sz_low = shift(sz_top, "gz", 1)
    sy_low = shift(sy_last, "gy", 1)
    (packed,) = call(packed_kernel, own, (ranks, flags), 8, 4000000)
    messages = [of((2 * len(zs) * rows, width), F32) for zs in plane_lists(depth)]
    both, partner, other, d_own, m_own = call(
        strength_kernel,
        messages + [of(ranks.shape, I32)] + own,
        (twice, rm, packed, sz_low, sy_low),
        8,
        4000000,
    )
    both = swap(both, "gz", 0)
    partner = swap(partner, "gz", 0)
    relayed = relay(both, "gz")
    other = swap(other, "gz", 1)
    message = of((y_layout(depth, True)[2], width), F32)
    yo, ye = call(early_kernel, [message, message], (d_own, m_own), 8, 1000000)
    ro1 = swap(yo, "gy", 1)
    re1 = swap(ye, "gy", 0)
    message = of((y_layout(depth, False)[2], width), F32)
    ext = (planes, rows, width)
    yo, ye, d_ext, m_ext = call(
        planes_kernel, [message, message, of(ext, I32), of(ext, F32)], (both, partner, other, relayed, d_own, m_own), 8, 4000000
    )
    ro2 = swap(yo, "gy", 1)
    re2 = swap(ye, "gy", 0)
    cells = (planes, width // L, rows + 2 * T, L)
    works = [of((STATE + ROUNDS,) + cells, F32), of((NEW + 1 + ROUNDS,) + cells, I32)]
    fw, iw = call(inner_kernel, works, (d_ext, m_ext), 8, 20000000)
    state, counts, _, _ = call(
        outer_kernel,
        [of(ranks.shape, I32), of((devices, 1, L), I32)] + works,
        (ro1, re1, ro2, re2, fw, iw),
        8,
        20000000,
        input_output_aliases={4: 2, 5: 3},
        out_specs=[pl.BlockSpec(memory_space=pl.ANY), vmem(), vmem(), vmem()],
        scratch_shapes=[pltpu.VMEM(ranks.shape, I32), pltpu.SemaphoreType.DMA((depth,))],
    )
    everyone = lax.all_to_all(counts, ("gz", "gy"), 0, 0, tiled=True)
    undecided = jnp.sum(everyone, axis=(0, 1))[:ROUNDS]
    return (state, undecided)


def solution(mesh):
    return jax.shard_map(
        per_device,
        mesh=mesh,
        in_specs=(P("gz", "gy", None), P(None, "gz", "gy", None), P("gz", "gy", None)),
        out_specs=(P("gz", "gy", None), P()),
        check_vma=False,
    )
```

```python
import jax
import jax.numpy as jnp
from jax import lax
from jax.experimental import pallas as pl
from jax.experimental.pallas import tpu as pltpu
from jax.sharding import PartitionSpec as P


ROUNDS = 3
H = 2 * ROUNDS
T = 8
RELAYED = 3
L = 128
BIG = 3.0e38
F32, I32 = jnp.float32, jnp.int32
CAPS, STATE, PATTERN, NEW = 0, 6, 0, 0


def vmem():
    return pl.BlockSpec(memory_space=pltpu.VMEM)


def neighbours(axis):
    i = lax.axis_index(axis)
    return i > 0, i < lax.axis_size(axis) - 1


def doubled(s):
    return jnp.where(s > 0, 2.0 * s, -1.0)


def scaled(p, bit):
    return jnp.where((bit != 0) & (p >= 0), 2.0 * p, p)


def edge_kernel(seeds, sz_top, sy_last, twice, rm):
    depth, rows, width = rm.shape
    _, zhi = neighbours("gz")
    _, yhi = neighbours("gy")
    shape = (rows, width)
    row = lax.broadcasted_iota(I32, shape, 0)
    x_in = lax.broadcasted_iota(I32, shape, 1) < width - 1
    y_in = (row < rows - 1) | yhi
    sz_top[...] = seeds[2, depth - 1]
    sz_prev = None
    for z in range(depth):
        sy_last[pl.ds(z, 1), :] = seeds[1, z, pl.ds(rows - 1, 1), :]
        sx = jnp.where(x_in, seeds[0, z], 0.0)
        sy = jnp.where(y_in, seeds[1, z], 0.0)
        sz = seeds[2, z]
        if z == depth - 1:
            sz = jnp.where(zhi, sz, 0.0)
        r = jnp.maximum(jnp.maximum(sx, pltpu.roll(sx, 1, 1)), jnp.maximum(sy, sz))
        r = jnp.maximum(r, jnp.where(row == 0, 0.0, pltpu.roll(sy, 1, 0)))
        rm[z] = r if z == 0 else jnp.maximum(r, sz_prev)
        sz_prev = sz
        for d, s in enumerate((sx, sy, sz)):
            twice[d, z] = doubled(s)


def plane_lists(depth):
    both = list(range(H - RELAYED, H))
    partner = [z for z in range(depth - H, depth) if z not in both]
    other = list(range(H - RELAYED))
    return both, partner, other


def shared_kernel(twice, rm, packed, sy_low, both, d_out, m_out):
    strength(twice, rm, packed, None, sy_low, (both,), d_out, m_out)


def strength_kernel(twice, rm, packed, sz_low, sy_low, partner, other, d_out, m_out):
    strength(twice, rm, packed, sz_low, sy_low, (None, partner, other), d_out, m_out)


def strength(twice, rm, packed, sz_low, sy_low, messages, d_out, m_out):
    depth, rows, width = packed.shape
    zlo, _ = neighbours("gz")
    ylo, _ = neighbours("gy")
    from_below = jnp.where(zlo, sz_low[...], 0.0) if sz_low is not None else jnp.zeros((rows, width), F32)
    row = lax.broadcasted_iota(I32, (rows, width), 0)
    tz_prev = doubled(from_below)
    for z in range(depth):
        sy_prev = jnp.where(ylo, sy_low[pl.ds(z, 1), :], 0.0)
        r = jnp.maximum(rm[z], jnp.where(row == 0, sy_prev, 0.0))
        if z == 0:
            r = jnp.maximum(r, from_below)
        tx, ty, tz = twice[0, z], twice[1, z], twice[2, z]
        ty_prev = jnp.where(row == 0, doubled(sy_prev), pltpu.roll(ty, 1, 0))
        d = jnp.where(tx >= r, 1, 0) + jnp.where(pltpu.roll(tx, 1, 1) >= r, 2, 0)
        d += jnp.where(ty >= r, 4, 0) + jnp.where(ty_prev >= r, 8, 0)
        d += jnp.where(tz >= r, 16, 0) + jnp.where(tz_prev >= r, 32, 0)
        d_out[z] = d
        tz_prev = tz
    for z in range(depth):
        d = d_out[z]
        i = (pltpu.roll(d, width - 1, 1) & 2) | (pltpu.roll(d, 1, 1) & 1)
        i |= jnp.where(row == rows - 1, 0, pltpu.roll(d, rows - 1, 0) & 8)
        i |= jnp.where(row == 0, 0, pltpu.roll(d, 1, 0) & 4)
        if z < depth - 1:
            i |= d_out[z + 1] & 32
        if z > 0:
            i |= d_out[z - 1] & 16
        pairs = (i & 21) + ((i >> 1) & 21)
        many = (pairs & 3) + ((pairs >> 2) & 3) + (pairs >> 4)
        p = packed[z]
        m = jnp.where(p >= 0, p * (1 << many).astype(F32), p)
        m_out[z] = m
    even = lax.axis_index("gz") % 2 == 0

    def send(place):
        for ref, zs in zip(messages, plane_lists(depth)):
            for j, z in enumerate(zs if ref is not None else ()):
                ref[pl.ds(j * rows, rows), :] = d_out[place(z)].astype(F32)
                ref[pl.ds((len(zs) + j) * rows, rows), :] = m_out[place(z)]

    @pl.when(even)
    def _():
        send(lambda z: z)

    @pl.when(jnp.logical_not(even))
    def _():
        send(lambda z: depth - 1 - z)


def y_layout(depth, early):
    patterns, measures, at = [], [], 0
    for out, least in ((patterns, 1), (measures, 0)):
        for z in range(-H, depth + H):
            k = max(-z, z - depth + 1, 0)
            n = max(H - k, least)
            ready = 0 <= z < depth and (least or 0 < z < depth - 1)
            if n and ready == early:
                out.append((z, n, at))
                at += n
    return patterns, measures, -(-at // T) * T


def send_rows(layout, pattern, measure, yo, ye):
    patterns, measures, _ = layout
    even = lax.axis_index("gy") % 2 == 0

    def send(upward, downward):
        for z, n, at in patterns:
            e = pattern(z).astype(F32)
            upward[pl.ds(at, n), :] = e[e.shape[0] - n :]
            downward[pl.ds(at, n), :] = e[:n]
        for z, n, at in measures:
            e = measure(z)
            upward[pl.ds(at, n), :] = e[e.shape[0] - n :]
            downward[pl.ds(at, n), :] = e[:n]

    @pl.when(even)
    def _():
        send(ye, yo)

    @pl.when(jnp.logical_not(even))
    def _():
        send(yo, ye)


def early_kernel(d_own, m_own, yo, ye):
    send_rows(y_layout(m_own.shape[0], True), lambda z: d_own[z], lambda z: m_own[z], yo, ye)


def planes_kernel(both, partner, other, relayed, d_own, m_own, yo, ye, d_ext, m_ext):
    depth, rows, _ = m_own.shape
    zlo, zhi = neighbours("gz")
    above = lax.axis_index("gz") % 2 == 0

    def put(ref, zs, above, distance):
        for j, z in enumerate(zs):
            k = distance(z)
            i = jnp.where(above, H + depth + k - 1, H - k)
            d = ref[pl.ds(j * rows, rows), :]
            d_ext[i] = jnp.where((above & zhi) | (jnp.logical_not(above) & zlo), d, 0.0).astype(I32)
            m_ext[i] = ref[pl.ds((len(zs) + j) * rows, rows), :]

    for_both, for_partner, for_other = plane_lists(depth)
    put(both, for_both, above, lambda z: depth - z)
    put(partner, for_partner, above, lambda z: depth - z)
    put(other, for_other, jnp.logical_not(above), lambda z: z + 1)
    put(relayed, for_both, jnp.logical_not(above), lambda z: z + 1)
    for z in range(depth):
        d_ext[H + z] = d_own[z]
        m_ext[H + z] = m_own[z]
    first, last = H, H + depth - 1
    m_ext[first - 1] = scaled(m_ext[first - 1], d_ext[first] & 32)
    m_ext[first] = scaled(m_ext[first], d_ext[first - 1] & 16)
    m_ext[last] = scaled(m_ext[last], d_ext[last + 1] & 32)
    m_ext[last + 1] = scaled(m_ext[last + 1], d_ext[last] & 16)
    send_rows(y_layout(depth, False), lambda z: d_ext[z + H], lambda z: m_ext[z + H], yo, ye)


def blocks(v):
    return jnp.stack([v[:, j : j + L] for j in range(0, v.shape[1], L)])


def x_next(v):
    r = pltpu.roll(v, L - 1, 2)
    lane = lax.broadcasted_iota(I32, v.shape, 2)
    return jnp.where(lane == L - 1, jnp.concatenate([r[1:], r[:1]], 0), r)


def x_prev(v):
    r = pltpu.roll(v, 1, 2)
    lane = lax.broadcasted_iota(I32, v.shape, 2)
    return jnp.where(lane == 0, jnp.concatenate([r[-1:], r[:-1]], 0), r)


def set_caps(fw, iw, sites):
    found = []
    for i, at in sites:

        def d_at(plane, row):
            return iw[PATTERN, plane, :, pl.ds(row, T), :]

        d = d_at(i, at)
        others = (x_next(d), x_prev(d), d_at(i, at + 1), d_at(i, at - 1), d_at(i + 1, at), d_at(i - 1, at))
        found.append([(d & (1 << j)) | (other & (1 << (j ^ 1))) for j, other in enumerate(others)])
    caps = [[jnp.where(linked != 0, BIG, -3.0) for linked in some] for some in found]
    for (i, at), some in zip(sites, caps):
        for j, cap in enumerate(some):
            fw[CAPS + j, i, :, pl.ds(at, T), :] = cap
    return caps


def caps_of(fw, sites):
    return [[fw[CAPS + j, i, :, pl.ds(at, T), :] for j in range(6)] for i, at in sites]


def select(fw, iw, step, sites, caps):
    found = []
    for (i, at), cap in zip(sites, caps):

        def p_at(plane, row):
            return fw[STATE + step, plane, :, pl.ds(row, T), :]

        p = p_at(i, at)
        y = jnp.maximum(jnp.minimum(p_at(i, at + 1), cap[2]), jnp.minimum(p_at(i, at - 1), cap[3]))
        z = jnp.maximum(jnp.minimum(p_at(i + 1, at), cap[4]), jnp.minimum(p_at(i - 1, at), cap[5]))
        x = jnp.maximum(jnp.minimum(x_next(p), cap[0]), jnp.minimum(x_prev(p), cap[1]))
        found.append((p >= 0) & (p > jnp.maximum(jnp.maximum(y, z), x)))
    for (i, at), new in zip(sites, found):
        iw[NEW + 1 + step, i, :, pl.ds(at, T), :] = jnp.where(new, 63, 0)


def hits(fw, iw, step, i, at):
    def n_at(plane, row):
        return iw[NEW + 1 + step, plane, :, pl.ds(row, T), :]

    new = n_at(i, at)
    hit = ((n_at(i, at + 1) & 4) | (n_at(i, at - 1) & 8)) | ((n_at(i + 1, at) & 16) | (n_at(i - 1, at) & 32))
    hit |= (x_next(new) & 1) | (x_prev(new) & 2)
    hit &= iw[PATTERN, i, :, pl.ds(at, T), :]
    return new != 0, hit != 0, fw[STATE + step, i, :, pl.ds(at, T), :]


def update(fw, iw, step, sites):
    found = []
    for i, at in sites:
        new, hit, p = hits(fw, iw, step, i, at)
        found.append(jnp.where(new, -2.0, jnp.where((p >= 0) & hit, -1.0, p)))
    for (i, at), p in zip(sites, found):
        fw[STATE + step + 1, i, :, pl.ds(at, T), :] = p


def stages(fw, iw, depth, rows_of):
    for stage in range(2 * ROUNDS - 1):
        step, reach = stage // 2, H - 1 - stage
        each = max(n for n in (1, 2, 3, 4) if (depth + 2 * reach) % n == 0)

        @pl.loop(H - reach, H + depth + reach, step=each)
        def _(i):
            sites = [(i + j, at) for j in range(each) for at in rows_of(stage)]
            if stage == 0:
                select(fw, iw, step, sites, set_caps(fw, iw, sites))
            elif stage % 2 == 0:
                select(fw, iw, step, sites, caps_of(fw, sites))
            else:
                update(fw, iw, step, sites)


def inner_kernel(d_ext, m_ext, fw, iw):
    planes, rows, _ = m_ext.shape
    depth = planes - 2 * H

    @pl.loop(0, planes)
    def _(i):
        iw[PATTERN, i, :, pl.ds(T, rows), :] = blocks(d_ext[i])
        fw[STATE, i, :, pl.ds(T, rows), :] = blocks(m_ext[i])

    stages(fw, iw, depth, lambda stage: range(T, T + rows, T))


def outer_kernel(ro1, re1, ro2, re2, fw_in, iw_in, state_out, count_out, fw, iw, state_ref, sems):
    del fw_in, iw_in
    depth, rows, width = state_ref.shape
    planes = depth + 2 * H
    ylo, yhi = neighbours("gy")
    even = lax.axis_index("gy") % 2 == 0
    for ro, re, early in ((ro1, re1, True), (ro2, re2, False)):
        patterns, measures, _ = y_layout(depth, early)
        for z, n, at in patterns:
            e, o = re[pl.ds(at, n), :], ro[pl.ds(at, n), :]
            above = jnp.where(yhi, jnp.where(even, e, o), 0.0).astype(I32)
            below = jnp.where(ylo, jnp.where(even, o, e), 0.0).astype(I32)
            iw[PATTERN, z + H, :, pl.ds(T - n, n), :] = blocks(below)
            iw[PATTERN, z + H, :, pl.ds(T + rows, n), :] = blocks(above)
        for z, n, at in measures:
            e, o = re[pl.ds(at, n), :], ro[pl.ds(at, n), :]
            fw[STATE, z + H, :, pl.ds(T - n, n), :] = blocks(jnp.where(even, o, e))
            fw[STATE, z + H, :, pl.ds(T + rows, n), :] = blocks(jnp.where(even, e, o))

    def low(stage):
        return T - H + stage

    def high(stage):
        return T + rows + H - T - stage

    shape = (width // L, T, L)
    row = lax.broadcasted_iota(I32, shape, 1)

    each = max(n for n in (1, 2, 4) if planes % n == 0)

    @pl.loop(0, planes, step=each)
    def _(i):
        sites = [(i + j, *edge) for j in range(each) for edge in ((low(0), H - 1, H), (high(0), T - H - 1, T - H))]
        found = []
        for i, at, one, two in sites:
            d_next = iw[PATTERN, i, :, pl.ds(at + 1, T), :]
            d_prev = iw[PATTERN, i, :, pl.ds(at - 1, T), :]
            bit = jnp.where(row == one, d_next & 8, jnp.where(row == two, d_prev & 4, 0))
            found.append(scaled(fw[STATE, i, :, pl.ds(at, T), :], bit))
        for (i, at, _, _), p in zip(sites, found):
            fw[STATE, i, :, pl.ds(at, T), :] = p

    stages(fw, iw, depth, lambda stage: (low(stage), high(stage)))

    def finish(z, totals):
        totals = list(totals)
        for at in range(0, rows, T):
            new, hit, p = hits(fw, iw, ROUNDS - 1, z + H, T + at)
            old = jnp.where(p >= 0, jnp.where(hit, 1, 0), jnp.where(p == -2.0, 2, 1))
            state = jnp.where(new, 2, old)
            for j in range(width // L):
                state_ref[z, pl.ds(at, T), pl.ds(j * L, L)] = state[j]
            totals[-1] = totals[-1] + jnp.where(state == 0, 1, 0)
            for step in range(ROUNDS - 1):
                p = fw[STATE + step + 1, z + H, :, pl.ds(T + at, T), :]
                totals[step] = totals[step] + jnp.where(p >= 0, 1, 0)
        pltpu.make_async_copy(state_ref.at[z], state_out.at[z], sems.at[z]).start()
        return tuple(totals)

    totals = lax.fori_loop(0, depth, finish, (jnp.zeros(shape, I32),) * ROUNDS)
    lane = lax.broadcasted_iota(I32, count_out.shape, 2)
    counts = jnp.zeros(count_out.shape, I32)
    for step in range(ROUNDS):
        counts = jnp.where(lane == step, jnp.sum(totals[step]), counts)
    count_out[...] = counts
    for z in range(depth):
        pltpu.make_async_copy(state_ref.at[z], state_out.at[z], sems.at[z]).wait()


def shift(value, axis, step):
    count = lax.axis_size(axis)
    return lax.ppermute(value, axis, [(i, (i + step) % count) for i in range(count)])


def swap(value, axis, odd):
    count = lax.axis_size(axis)
    pairs = [(i, i) for i in range(count)]
    for i in range(odd, count - 1, 2):
        pairs[i], pairs[i + 1] = (i, i + 1), (i + 1, i)
    return lax.ppermute(value, axis, pairs)


def relay(value, axis):
    last = lax.axis_size(axis) - 1
    pairs = [(i, min(i + 2, last) if i % 2 == 0 else max(i - 2, 0)) for i in range(last + 1)]
    return lax.ppermute(value, axis, pairs)


def call(kernel, outs, args, limit, cost, **more):
    return pl.pallas_call(
        kernel,
        out_shape=outs,
        in_specs=[vmem()] * len(args),
        out_specs=more.pop("out_specs", [vmem()] * len(outs)),
        compiler_params=pltpu.CompilerParams(vmem_limit_bytes=limit * 2**20),
        cost_estimate=pl.CostEstimate(flops=cost, bytes_accessed=cost, transcendentals=0),
        **more,
    )(*args)


def per_device(ranks, seeds, flags):
    depth, rows, width = ranks.shape
    assert RELAYED <= 2 * H - depth and H < depth and lax.axis_size("gz") % 2 == 0 and rows >= 2 * T and T == H + 2 and width % L == 0
    planes = depth + 2 * H
    devices = lax.axis_size("gz") * lax.axis_size("gy")
    of = jax.ShapeDtypeStruct
    own = [of(ranks.shape, F32)]
    sz_top, sy_last, twice, rm = call(
        edge_kernel,
        [of((rows, width), F32), of((depth, width), F32), of(seeds.shape, F32)] + own,
        (seeds,),
        8,
        4000000,
    )
    sy_low = shift(sy_last, "gy", 1)
    sz_low = shift(sz_top, "gz", 1)
    packed = jnp.where(flags == 0, ranks, jnp.where(flags == 2, -2.0, -1.0))
    messages = [of((2 * len(zs) * rows, width), F32) for zs in plane_lists(depth)]
    cells = [of(ranks.shape, I32)] + own
    scratch = [pltpu.VMEM(ranks.shape, I32), pltpu.VMEM(ranks.shape, F32)]
    (both,) = call(shared_kernel, messages[:1], (twice, rm, packed, sy_low), 8, 4000000, scratch_shapes=scratch)
    both = swap(both, "gz", 0)
    partner, other, d_own, m_own = call(
        strength_kernel, messages[1:] + cells, (twice, rm, packed, sz_low, sy_low), 8, 4000000
    )
    partner = swap(partner, "gz", 0)
    relayed = relay(both, "gz")
    other = swap(other, "gz", 1)
    message = of((y_layout(depth, True)[2], width), F32)
    yo, ye = call(early_kernel, [message, message], (d_own, m_own), 8, 1000000)
    ro1 = swap(yo, "gy", 1)
    re1 = swap(ye, "gy", 0)
    message = of((y_layout(depth, False)[2], width), F32)
    ext = (planes, rows, width)
    yo, ye, d_ext, m_ext = call(
        planes_kernel, [message, message, of(ext, I32), of(ext, F32)], (both, partner, other, relayed, d_own, m_own), 8, 4000000
    )
    ro2 = swap(yo, "gy", 1)
    re2 = swap(ye, "gy", 0)
    cells = (planes, width // L, rows + 2 * T, L)
    works = [of((STATE + ROUNDS,) + cells, F32), of((NEW + 1 + ROUNDS,) + cells, I32)]
    fw, iw = call(inner_kernel, works, (d_ext, m_ext), 8, 20000000)
    state, counts, _, _ = call(
        outer_kernel,
        [of(ranks.shape, I32), of((devices, 1, L), I32)] + works,
        (ro1, re1, ro2, re2, fw, iw),
        8,
        20000000,
        input_output_aliases={4: 2, 5: 3},
        out_specs=[pl.BlockSpec(memory_space=pl.ANY), vmem(), vmem(), vmem()],
        scratch_shapes=[pltpu.VMEM(ranks.shape, I32), pltpu.SemaphoreType.DMA((depth,))],
    )
    everyone = lax.all_to_all(counts, ("gz", "gy"), 0, 0, tiled=True)
    undecided = jnp.sum(everyone, axis=(0, 1))[:ROUNDS]
    return (state, undecided)


def solution(mesh):
    return jax.shard_map(
        per_device,
        mesh=mesh,
        in_specs=(P("gz", "gy", None), P(None, "gz", "gy", None), P("gz", "gy", None)),
        out_specs=(P("gz", "gy", None), P()),
        check_vma=False,
    )
```

```python
import jax
import jax.numpy as jnp
from jax import lax
from jax.experimental import pallas as pl
from jax.experimental.pallas import tpu as pltpu
from jax.sharding import PartitionSpec as P


ROUNDS = 3
H = 2 * ROUNDS
T = 8
RELAYED = 3
L = 128
BIG = 3.0e38
F32, I32 = jnp.float32, jnp.int32
CAPS, STATE, PATTERN, NEW = 0, 6, 0, 0


def vmem():
    return pl.BlockSpec(memory_space=pltpu.VMEM)


def neighbours(axis):
    i = lax.axis_index(axis)
    return i > 0, i < lax.axis_size(axis) - 1


def doubled(s):
    return jnp.where(s > 0, 2.0 * s, -1.0)


def scaled(p, bit):
    return jnp.where((bit != 0) & (p >= 0), 2.0 * p, p)


def edge_kernel(seeds, sz_top, sy_last, twice, rm):
    depth, rows, width = rm.shape
    _, zhi = neighbours("gz")
    _, yhi = neighbours("gy")
    shape = (rows, width)
    row = lax.broadcasted_iota(I32, shape, 0)
    x_in = lax.broadcasted_iota(I32, shape, 1) < width - 1
    y_in = (row < rows - 1) | yhi
    sz_top[...] = seeds[2, depth - 1]
    sz_prev = None
    for z in range(depth):
        sy_last[pl.ds(z, 1), :] = seeds[1, z, pl.ds(rows - 1, 1), :]
        sx = jnp.where(x_in, seeds[0, z], 0.0)
        sy = jnp.where(y_in, seeds[1, z], 0.0)
        sz = seeds[2, z]
        if z == depth - 1:
            sz = jnp.where(zhi, sz, 0.0)
        r = jnp.maximum(jnp.maximum(sx, pltpu.roll(sx, 1, 1)), jnp.maximum(sy, sz))
        r = jnp.maximum(r, jnp.where(row == 0, 0.0, pltpu.roll(sy, 1, 0)))
        rm[z] = r if z == 0 else jnp.maximum(r, sz_prev)
        sz_prev = sz
        for d, s in enumerate((sx, sy, sz)):
            twice[d, z] = doubled(s)


def plane_lists(depth):
    both = list(range(H - RELAYED, H))
    partner = [z for z in range(depth - H, depth) if z not in both]
    other = list(range(H - RELAYED))
    return both, partner, other


def shared_kernel(twice, rm, packed, sy_low, both, d_out, m_out):
    strength(twice, rm, packed, None, sy_low, (both,), d_out, m_out)


def strength_kernel(twice, rm, packed, sz_low, sy_low, partner, other, d_out, m_out):
    strength(twice, rm, packed, sz_low, sy_low, (None, partner, other), d_out, m_out)


def strength(twice, rm, packed, sz_low, sy_low, messages, d_out, m_out):
    depth, rows, width = packed.shape
    zlo, _ = neighbours("gz")
    ylo, _ = neighbours("gy")
    from_below = jnp.where(zlo, sz_low[...], 0.0) if sz_low is not None else jnp.zeros((rows, width), F32)
    row = lax.broadcasted_iota(I32, (rows, width), 0)
    tz_prev = doubled(from_below)
    for z in range(depth):
        sy_prev = jnp.where(ylo, sy_low[pl.ds(z, 1), :], 0.0)
        r = jnp.maximum(rm[z], jnp.where(row == 0, sy_prev, 0.0))
        if z == 0:
            r = jnp.maximum(r, from_below)
        tx, ty, tz = twice[0, z], twice[1, z], twice[2, z]
        ty_prev = jnp.where(row == 0, doubled(sy_prev), pltpu.roll(ty, 1, 0))
        d = jnp.where(tx >= r, 1, 0) + jnp.where(pltpu.roll(tx, 1, 1) >= r, 2, 0)
        d += jnp.where(ty >= r, 4, 0) + jnp.where(ty_prev >= r, 8, 0)
        d += jnp.where(tz >= r, 16, 0) + jnp.where(tz_prev >= r, 32, 0)
        d_out[z] = d
        tz_prev = tz
    for z in range(depth):
        d = d_out[z]
        i = (pltpu.roll(d, width - 1, 1) & 2) | (pltpu.roll(d, 1, 1) & 1)
        i |= jnp.where(row == rows - 1, 0, pltpu.roll(d, rows - 1, 0) & 8)
        i |= jnp.where(row == 0, 0, pltpu.roll(d, 1, 0) & 4)
        if z < depth - 1:
            i |= d_out[z + 1] & 32
        if z > 0:
            i |= d_out[z - 1] & 16
        pairs = (i & 21) + ((i >> 1) & 21)
        many = (pairs & 3) + ((pairs >> 2) & 3) + (pairs >> 4)
        p = packed[z]
        m = jnp.where(p >= 0, p * (1 << many).astype(F32), p)
        m_out[z] = m
    even = lax.axis_index("gz") % 2 == 0

    def send(place):
        for ref, zs in zip(messages, plane_lists(depth)):
            for j, z in enumerate(zs if ref is not None else ()):
                ref[pl.ds(j * rows, rows), :] = d_out[place(z)].astype(F32)
                ref[pl.ds((len(zs) + j) * rows, rows), :] = m_out[place(z)]

    @pl.when(even)
    def _():
        send(lambda z: z)

    @pl.when(jnp.logical_not(even))
    def _():
        send(lambda z: depth - 1 - z)


def y_layout(depth, early):
    patterns, measures, at = [], [], 0
    for out, least in ((patterns, 1), (measures, 0)):
        for z in range(-H, depth + H):
            k = max(-z, z - depth + 1, 0)
            n = max(H - k, least)
            ready = 0 <= z < depth and (least or 0 < z < depth - 1)
            if n and ready == early:
                out.append((z, n, at))
                at += n
    return patterns, measures, -(-at // T) * T


def send_rows(layout, pattern, measure, yo, ye):
    patterns, measures, _ = layout
    even = lax.axis_index("gy") % 2 == 0

    def send(upward, downward):
        for z, n, at in patterns:
            e = pattern(z).astype(F32)
            upward[pl.ds(at, n), :] = e[e.shape[0] - n :]
            downward[pl.ds(at, n), :] = e[:n]
        for z, n, at in measures:
            e = measure(z)
            upward[pl.ds(at, n), :] = e[e.shape[0] - n :]
            downward[pl.ds(at, n), :] = e[:n]

    @pl.when(even)
    def _():
        send(ye, yo)

    @pl.when(jnp.logical_not(even))
    def _():
        send(yo, ye)


def early_kernel(d_own, m_own, yo, ye):
    send_rows(y_layout(m_own.shape[0], True), lambda z: d_own[z], lambda z: m_own[z], yo, ye)


def planes_kernel(both, partner, other, relayed, d_own, m_own, yo, ye, d_ext, m_ext):
    depth, rows, _ = m_own.shape
    zlo, zhi = neighbours("gz")
    above = lax.axis_index("gz") % 2 == 0

    def put(ref, zs, above, distance):
        for j, z in enumerate(zs):
            k = distance(z)
            i = jnp.where(above, H + depth + k - 1, H - k)
            d = ref[pl.ds(j * rows, rows), :]
            d_ext[i] = jnp.where((above & zhi) | (jnp.logical_not(above) & zlo), d, 0.0).astype(I32)
            m_ext[i] = ref[pl.ds((len(zs) + j) * rows, rows), :]

    for_both, for_partner, for_other = plane_lists(depth)
    put(both, for_both, above, lambda z: depth - z)
    put(partner, for_partner, above, lambda z: depth - z)
    put(other, for_other, jnp.logical_not(above), lambda z: z + 1)
    put(relayed, for_both, jnp.logical_not(above), lambda z: z + 1)
    for z in range(depth):
        d_ext[H + z] = d_own[z]
        m_ext[H + z] = m_own[z]
    first, last = H, H + depth - 1
    m_ext[first - 1] = scaled(m_ext[first - 1], d_ext[first] & 32)
    m_ext[first] = scaled(m_ext[first], d_ext[first - 1] & 16)
    m_ext[last] = scaled(m_ext[last], d_ext[last + 1] & 32)
    m_ext[last + 1] = scaled(m_ext[last + 1], d_ext[last] & 16)
    send_rows(y_layout(depth, False), lambda z: d_ext[z + H], lambda z: m_ext[z + H], yo, ye)


def blocks(v):
    return jnp.stack([v[:, j : j + L] for j in range(0, v.shape[1], L)])


def x_next(v):
    r = pltpu.roll(v, L - 1, 2)
    lane = lax.broadcasted_iota(I32, v.shape, 2)
    return jnp.where(lane == L - 1, jnp.concatenate([r[1:], r[:1]], 0), r)


def x_prev(v):
    r = pltpu.roll(v, 1, 2)
    lane = lax.broadcasted_iota(I32, v.shape, 2)
    return jnp.where(lane == 0, jnp.concatenate([r[-1:], r[:-1]], 0), r)


def set_caps(fw, iw, sites):
    found = []
    for i, at in sites:

        def d_at(plane, row):
            return iw[PATTERN, plane, :, pl.ds(row, T), :]

        d = d_at(i, at)
        others = (x_next(d), x_prev(d), d_at(i, at + 1), d_at(i, at - 1), d_at(i + 1, at), d_at(i - 1, at))
        found.append([(d & (1 << j)) | (other & (1 << (j ^ 1))) for j, other in enumerate(others)])
    caps = [[jnp.where(linked != 0, BIG, -3.0) for linked in some] for some in found]
    for (i, at), some in zip(sites, caps):
        for j, cap in enumerate(some):
            fw[CAPS + j, i, :, pl.ds(at, T), :] = cap
    return caps


def caps_of(fw, sites):
    return [[fw[CAPS + j, i, :, pl.ds(at, T), :] for j in range(6)] for i, at in sites]


def select(fw, iw, step, sites, caps):
    found = []
    for (i, at), cap in zip(sites, caps):

        def p_at(plane, row):
            return fw[STATE + step, plane, :, pl.ds(row, T), :]

        p = p_at(i, at)
        y = jnp.maximum(jnp.minimum(p_at(i, at + 1), cap[2]), jnp.minimum(p_at(i, at - 1), cap[3]))
        z = jnp.maximum(jnp.minimum(p_at(i + 1, at), cap[4]), jnp.minimum(p_at(i - 1, at), cap[5]))
        x = jnp.maximum(jnp.minimum(x_next(p), cap[0]), jnp.minimum(x_prev(p), cap[1]))
        found.append((p >= 0) & (p > jnp.maximum(jnp.maximum(y, z), x)))
    for (i, at), new in zip(sites, found):
        iw[NEW + 1 + step, i, :, pl.ds(at, T), :] = jnp.where(new, 63, 0)


def hits(fw, iw, step, i, at):
    def n_at(plane, row):
        return iw[NEW + 1 + step, plane, :, pl.ds(row, T), :]

    new = n_at(i, at)
    hit = ((n_at(i, at + 1) & 4) | (n_at(i, at - 1) & 8)) | ((n_at(i + 1, at) & 16) | (n_at(i - 1, at) & 32))
    hit |= (x_next(new) & 1) | (x_prev(new) & 2)
    hit &= iw[PATTERN, i, :, pl.ds(at, T), :]
    return new != 0, hit != 0, fw[STATE + step, i, :, pl.ds(at, T), :]


def update(fw, iw, step, sites):
    found = []
    for i, at in sites:
        new, hit, p = hits(fw, iw, step, i, at)
        found.append(jnp.where(new, -2.0, jnp.where((p >= 0) & hit, -1.0, p)))
    for (i, at), p in zip(sites, found):
        fw[STATE + step + 1, i, :, pl.ds(at, T), :] = p


def stages(fw, iw, depth, rows_of):
    for stage in range(2 * ROUNDS - 1):
        step, reach = stage // 2, H - 1 - stage

        def planes(i, each):
            sites = [(i + j, at) for j in range(each) for at in rows_of(stage)]
            if stage == 0:
                select(fw, iw, step, sites, set_caps(fw, iw, sites))
            elif stage % 2 == 0:
                select(fw, iw, step, sites, caps_of(fw, sites))
            else:
                update(fw, iw, step, sites)

        first, count = H - reach, depth + 2 * reach
        each = 3 if stage == 0 and count % 3 == 0 else 4
        whole_steps = count // each * each

        @pl.loop(first, first + whole_steps, step=each)
        def _(i):
            planes(i, each)

        if count > whole_steps:
            planes(first + whole_steps, count - whole_steps)


def inner_kernel(d_ext, m_ext, fw, iw):
    planes, rows, _ = m_ext.shape
    depth = planes - 2 * H

    @pl.loop(0, planes)
    def _(i):
        iw[PATTERN, i, :, pl.ds(T, rows), :] = blocks(d_ext[i])
        fw[STATE, i, :, pl.ds(T, rows), :] = blocks(m_ext[i])

    stages(fw, iw, depth, lambda stage: range(T, T + rows, T))


def outer_kernel(ro1, re1, ro2, re2, fw_in, iw_in, state_out, count_out, fw, iw, state_ref, sems):
    del fw_in, iw_in
    depth, rows, width = state_ref.shape
    planes = depth + 2 * H
    ylo, yhi = neighbours("gy")
    even = lax.axis_index("gy") % 2 == 0

    def unpack(above, below, early):
        patterns, measures, _ = y_layout(depth, early)
        for z, n, at in patterns:
            d = jnp.where(yhi, above[pl.ds(at, n), :], 0.0).astype(I32)
            iw[PATTERN, z + H, :, pl.ds(T + rows, n), :] = blocks(d)
            d = jnp.where(ylo, below[pl.ds(at, n), :], 0.0).astype(I32)
            iw[PATTERN, z + H, :, pl.ds(T - n, n), :] = blocks(d)
        for z, n, at in measures:
            fw[STATE, z + H, :, pl.ds(T + rows, n), :] = blocks(above[pl.ds(at, n), :])
            fw[STATE, z + H, :, pl.ds(T - n, n), :] = blocks(below[pl.ds(at, n), :])

    @pl.when(even)
    def _():
        unpack(re1, ro1, True)
        unpack(re2, ro2, False)

    @pl.when(jnp.logical_not(even))
    def _():
        unpack(ro1, re1, True)
        unpack(ro2, re2, False)

    def low(stage):
        return T - H + stage

    def high(stage):
        return T + rows + H - T - stage

    shape = (width // L, T, L)
    row = lax.broadcasted_iota(I32, shape, 1)

    each = max(n for n in (1, 2, 4) if planes % n == 0)

    @pl.loop(0, planes, step=each)
    def _(i):
        sites = [(i + j, *edge) for j in range(each) for edge in ((low(0), H - 1, H), (high(0), T - H - 1, T - H))]
        found = []
        for i, at, one, two in sites:
            d_next = iw[PATTERN, i, :, pl.ds(at + 1, T), :]
            d_prev = iw[PATTERN, i, :, pl.ds(at - 1, T), :]
            bit = jnp.where(row == one, d_next & 8, jnp.where(row == two, d_prev & 4, 0))
            found.append(scaled(fw[STATE, i, :, pl.ds(at, T), :], bit))
        for (i, at, _, _), p in zip(sites, found):
            fw[STATE, i, :, pl.ds(at, T), :] = p

    stages(fw, iw, depth, lambda stage: (low(stage), high(stage)))

    def finish(z, totals):
        totals = list(totals)
        for at in range(0, rows, T):
            new, hit, p = hits(fw, iw, ROUNDS - 1, z + H, T + at)
            old = jnp.where(p >= 0, jnp.where(hit, 1, 0), jnp.where(p == -2.0, 2, 1))
            state = jnp.where(new, 2, old)
            for j in range(width // L):
                state_ref[z, pl.ds(at, T), pl.ds(j * L, L)] = state[j]
            totals[-1] = totals[-1] + jnp.where(state == 0, 1, 0)
            for step in range(ROUNDS - 1):
                p = fw[STATE + step + 1, z + H, :, pl.ds(T + at, T), :]
                totals[step] = totals[step] + jnp.where(p >= 0, 1, 0)
        pltpu.make_async_copy(state_ref.at[z], state_out.at[z], sems.at[z]).start()
        return tuple(totals)

    totals = lax.fori_loop(0, depth, finish, (jnp.zeros(shape, I32),) * ROUNDS, unroll=2 - depth % 2)
    row = lax.broadcasted_iota(I32, (T, L), 0)
    lane = lax.broadcasted_iota(I32, (T, L), 1)
    partial = jnp.zeros((T, L), I32)
    for step in range(ROUNDS):
        partial = jnp.where(row == step, jnp.sum(jnp.sum(totals[step], axis=0), axis=0, keepdims=True), partial)
    counts = jnp.where(lane == row, jnp.sum(partial, axis=1, keepdims=True), 0)
    counts = jnp.sum(counts, axis=0, keepdims=True)
    count_out[...] = jnp.broadcast_to(counts[None], count_out.shape)
    for z in range(depth):
        pltpu.make_async_copy(state_ref.at[z], state_out.at[z], sems.at[z]).wait()


def shift(value, axis, step):
    count = lax.axis_size(axis)
    return lax.ppermute(value, axis, [(i, (i + step) % count) for i in range(count)])


def swap(value, axis, odd):
    count = lax.axis_size(axis)
    pairs = [(i, i) for i in range(count)]
    for i in range(odd, count - 1, 2):
        pairs[i], pairs[i + 1] = (i, i + 1), (i + 1, i)
    return lax.ppermute(value, axis, pairs)


def relay(value, axis):
    last = lax.axis_size(axis) - 1
    pairs = [(i, min(i + 2, last) if i % 2 == 0 else max(i - 2, 0)) for i in range(last + 1)]
    return lax.ppermute(value, axis, pairs)


def call(kernel, outs, args, limit, cost, **more):
    return pl.pallas_call(
        kernel,
        out_shape=outs,
        in_specs=[vmem()] * len(args),
        out_specs=more.pop("out_specs", [vmem()] * len(outs)),
        compiler_params=pltpu.CompilerParams(vmem_limit_bytes=limit * 2**20),
        cost_estimate=pl.CostEstimate(flops=cost, bytes_accessed=cost, transcendentals=0),
        **more,
    )(*args)


def per_device(ranks, seeds, flags):
    depth, rows, width = ranks.shape
    assert RELAYED <= 2 * H - depth and H < depth and lax.axis_size("gz") % 2 == 0 and rows >= 2 * T and T == H + 2 and width % L == 0
    planes = depth + 2 * H
    devices = lax.axis_size("gz") * lax.axis_size("gy")
    of = jax.ShapeDtypeStruct
    own = [of(ranks.shape, F32)]
    sz_top, sy_last, twice, rm = call(
        edge_kernel,
        [of((rows, width), F32), of((depth, width), F32), of(seeds.shape, F32)] + own,
        (seeds,),
        8,
        4000000,
    )
    sy_low = shift(sy_last, "gy", 1)
    sz_low = shift(sz_top, "gz", 1)
    packed = jnp.where(flags == 0, ranks, jnp.where(flags == 2, -2.0, -1.0))
    messages = [of((2 * len(zs) * rows, width), F32) for zs in plane_lists(depth)]
    cells = [of(ranks.shape, I32)] + own
    scratch = [pltpu.VMEM(ranks.shape, I32), pltpu.VMEM(ranks.shape, F32)]
    (both,) = call(shared_kernel, messages[:1], (twice, rm, packed, sy_low), 8, 4000000, scratch_shapes=scratch)
    both = swap(both, "gz", 0)
    partner, other, d_own, m_own = call(
        strength_kernel, messages[1:] + cells, (twice, rm, packed, sz_low, sy_low), 8, 4000000
    )
    partner = swap(partner, "gz", 0)
    relayed = relay(both, "gz")
    other = swap(other, "gz", 1)
    message = of((y_layout(depth, True)[2], width), F32)
    yo, ye = call(early_kernel, [message, message], (d_own, m_own), 8, 1000000)
    ro1 = swap(yo, "gy", 1)
    re1 = swap(ye, "gy", 0)
    message = of((y_layout(depth, False)[2], width), F32)
    ext = (planes, rows, width)
    yo, ye, d_ext, m_ext = call(
        planes_kernel, [message, message, of(ext, I32), of(ext, F32)], (both, partner, other, relayed, d_own, m_own), 8, 4000000
    )
    ro2 = swap(yo, "gy", 1)
    re2 = swap(ye, "gy", 0)
    cells = (planes, width // L, rows + 2 * T, L)
    works = [of((STATE + ROUNDS,) + cells, F32), of((NEW + 1 + ROUNDS,) + cells, I32)]
    fw, iw = call(inner_kernel, works, (d_ext, m_ext), 8, 20000000)
    state, counts, _, _ = call(
        outer_kernel,
        [of(ranks.shape, I32), of((devices, 1, L), I32)] + works,
        (ro1, re1, ro2, re2, fw, iw),
        8,
        20000000,
        input_output_aliases={4: 2, 5: 3},
        out_specs=[pl.BlockSpec(memory_space=pl.ANY), vmem(), vmem(), vmem()],
        scratch_shapes=[pltpu.VMEM(ranks.shape, I32), pltpu.SemaphoreType.DMA((depth,))],
    )
    everyone = lax.all_to_all(counts, ("gz", "gy"), 0, 0, tiled=True)
    undecided = jnp.sum(everyone, axis=(0, 1))[:ROUNDS]
    return (state, undecided)


def solution(mesh):
    return jax.shard_map(
        per_device,
        mesh=mesh,
        in_specs=(P("gz", "gy", None), P(None, "gz", "gy", None), P("gz", "gy", None)),
        out_specs=(P("gz", "gy", None), P()),
        check_vma=False,
    )
```

```python
import jax
import jax.numpy as jnp
from jax import lax
from jax.experimental import pallas as pl
from jax.experimental.pallas import tpu as pltpu
from jax.sharding import PartitionSpec as P


ROUNDS = 3
H = 2 * ROUNDS
T = 8
RELAYED = 3
L = 128
BIG = 3.0e38
F32, I32 = jnp.float32, jnp.int32
CAPS, STATE, PATTERN, NEW = 0, 6, 0, 0


def vmem():
    return pl.BlockSpec(memory_space=pltpu.VMEM)


def neighbours(axis):
    i = lax.axis_index(axis)
    return i > 0, i < lax.axis_size(axis) - 1


def doubled(s):
    return jnp.where(s > 0, 2.0 * s, -1.0)


def scaled(p, bit):
    return jnp.where((bit != 0) & (p >= 0), 2.0 * p, p)


def edge_kernel(seeds, sz_top, sy_last, twice, rm):
    depth, rows, width = rm.shape
    _, zhi = neighbours("gz")
    _, yhi = neighbours("gy")
    shape = (rows, width)
    row = lax.broadcasted_iota(I32, shape, 0)
    x_in = lax.broadcasted_iota(I32, shape, 1) < width - 1
    y_in = (row < rows - 1) | yhi
    sz_top[...] = seeds[2, depth - 1]
    sz_prev = None
    for z in range(depth):
        sy_last[pl.ds(z, 1), :] = seeds[1, z, pl.ds(rows - 1, 1), :]
        sx = jnp.where(x_in, seeds[0, z], 0.0)
        sy = jnp.where(y_in, seeds[1, z], 0.0)
        sz = seeds[2, z]
        if z == depth - 1:
            sz = jnp.where(zhi, sz, 0.0)
        r = jnp.maximum(jnp.maximum(sx, pltpu.roll(sx, 1, 1)), jnp.maximum(sy, sz))
        r = jnp.maximum(r, jnp.where(row == 0, 0.0, pltpu.roll(sy, 1, 0)))
        rm[z] = r if z == 0 else jnp.maximum(r, sz_prev)
        sz_prev = sz
        for d, s in enumerate((sx, sy, sz)):
            twice[d, z] = doubled(s)


def plane_lists(depth):
    both = list(range(H - RELAYED, H))
    partner = [z for z in range(depth - H, depth) if z not in both]
    other = list(range(H - RELAYED))
    return both, partner, other


def shared_kernel(twice, rm, packed, sy_low, both, d_out, m_out):
    strength(twice, rm, packed, None, sy_low, (both,), d_out, m_out)


def strength_kernel(twice, rm, packed, sz_low, sy_low, partner, other, d_out, m_out):
    strength(twice, rm, packed, sz_low, sy_low, (None, partner, other), d_out, m_out)


def strength(twice, rm, packed, sz_low, sy_low, messages, d_out, m_out):
    depth, rows, width = packed.shape
    zlo, _ = neighbours("gz")
    ylo, _ = neighbours("gy")
    from_below = jnp.where(zlo, sz_low[...], 0.0) if sz_low is not None else jnp.zeros((rows, width), F32)
    row = lax.broadcasted_iota(I32, (rows, width), 0)
    ms = range(depth) if sz_low is not None else range(depth - H, H)
    ds = range(max(ms[0] - 1, 0), min(ms[-1] + 2, depth))
    tz_prev = doubled(from_below) if ds[0] == 0 else twice[2, ds[0] - 1]
    for z in ds:
        sy_prev = jnp.where(ylo, sy_low[pl.ds(z, 1), :], 0.0)
        r = jnp.maximum(rm[z], jnp.where(row == 0, sy_prev, 0.0))
        if z == 0:
            r = jnp.maximum(r, from_below)
        tx, ty, tz = twice[0, z], twice[1, z], twice[2, z]
        ty_prev = jnp.where(row == 0, doubled(sy_prev), pltpu.roll(ty, 1, 0))
        d = jnp.where(tx >= r, 1, 0) + jnp.where(pltpu.roll(tx, 1, 1) >= r, 2, 0)
        d += jnp.where(ty >= r, 4, 0) + jnp.where(ty_prev >= r, 8, 0)
        d += jnp.where(tz >= r, 16, 0) + jnp.where(tz_prev >= r, 32, 0)
        d_out[z] = d
        tz_prev = tz
    for z in ms:
        d = d_out[z]
        i = (pltpu.roll(d, width - 1, 1) & 2) | (pltpu.roll(d, 1, 1) & 1)
        i |= jnp.where(row == rows - 1, 0, pltpu.roll(d, rows - 1, 0) & 8)
        i |= jnp.where(row == 0, 0, pltpu.roll(d, 1, 0) & 4)
        if z < depth - 1:
            i |= d_out[z + 1] & 32
        if z > 0:
            i |= d_out[z - 1] & 16
        pairs = (i & 21) + ((i >> 1) & 21)
        many = (pairs & 3) + ((pairs >> 2) & 3) + (pairs >> 4)
        p = packed[z]
        m = jnp.where(p >= 0, p * (1 << many).astype(F32), p)
        m_out[z] = m
    even = lax.axis_index("gz") % 2 == 0

    def send(place):
        for ref, zs in zip(messages, plane_lists(depth)):
            for j, z in enumerate(zs if ref is not None else ()):
                ref[pl.ds(j * rows, rows), :] = d_out[place(z)].astype(F32)
                ref[pl.ds((len(zs) + j) * rows, rows), :] = m_out[place(z)]

    @pl.when(even)
    def _():
        send(lambda z: z)

    @pl.when(jnp.logical_not(even))
    def _():
        send(lambda z: depth - 1 - z)


def y_layout(depth, early):
    patterns, measures, at = [], [], 0
    for out, least in ((patterns, 1), (measures, 0)):
        for z in range(-H, depth + H):
            k = max(-z, z - depth + 1, 0)
            n = max(H - k, least)
            ready = 0 <= z < depth and (least or 0 < z < depth - 1)
            if n and ready == early:
                out.append((z, n, at))
                at += n
    return patterns, measures, -(-at // T) * T


def send_rows(layout, pattern, measure, yo, ye):
    patterns, measures, _ = layout
    even = lax.axis_index("gy") % 2 == 0

    def send(upward, downward):
        for z, n, at in patterns:
            e = pattern(z).astype(F32)
            upward[pl.ds(at, n), :] = e[e.shape[0] - n :]
            downward[pl.ds(at, n), :] = e[:n]
        for z, n, at in measures:
            e = measure(z)
            upward[pl.ds(at, n), :] = e[e.shape[0] - n :]
            downward[pl.ds(at, n), :] = e[:n]

    @pl.when(even)
    def _():
        send(ye, yo)

    @pl.when(jnp.logical_not(even))
    def _():
        send(yo, ye)


def early_kernel(d_own, m_own, yo, ye):
    send_rows(y_layout(m_own.shape[0], True), lambda z: d_own[z], lambda z: m_own[z], yo, ye)


def planes_kernel(both, partner, other, relayed, d_own, m_own, yo, ye, d_ext, m_ext):
    depth, rows, _ = m_own.shape
    zlo, zhi = neighbours("gz")
    above = lax.axis_index("gz") % 2 == 0

    def put(ref, zs, above, distance):
        for j, z in enumerate(zs):
            k = distance(z)
            i = jnp.where(above, H + depth + k - 1, H - k)
            d = ref[pl.ds(j * rows, rows), :]
            d_ext[i] = jnp.where((above & zhi) | (jnp.logical_not(above) & zlo), d, 0.0).astype(I32)
            m_ext[i] = ref[pl.ds((len(zs) + j) * rows, rows), :]

    for_both, for_partner, for_other = plane_lists(depth)
    put(both, for_both, above, lambda z: depth - z)
    put(partner, for_partner, above, lambda z: depth - z)
    put(other, for_other, jnp.logical_not(above), lambda z: z + 1)
    put(relayed, for_both, jnp.logical_not(above), lambda z: z + 1)
    for z in range(depth):
        d_ext[H + z] = d_own[z]
        m_ext[H + z] = m_own[z]
    first, last = H, H + depth - 1
    m_ext[first - 1] = scaled(m_ext[first - 1], d_ext[first] & 32)
    m_ext[first] = scaled(m_ext[first], d_ext[first - 1] & 16)
    m_ext[last] = scaled(m_ext[last], d_ext[last + 1] & 32)
    m_ext[last + 1] = scaled(m_ext[last + 1], d_ext[last] & 16)
    send_rows(y_layout(depth, False), lambda z: d_ext[z + H], lambda z: m_ext[z + H], yo, ye)


def blocks(v):
    return jnp.stack([v[:, j : j + L] for j in range(0, v.shape[1], L)])


def x_next(v):
    r = pltpu.roll(v, L - 1, 2)
    lane = lax.broadcasted_iota(I32, v.shape, 2)
    return jnp.where(lane == L - 1, jnp.concatenate([r[1:], r[:1]], 0), r)


def x_prev(v):
    r = pltpu.roll(v, 1, 2)
    lane = lax.broadcasted_iota(I32, v.shape, 2)
    return jnp.where(lane == 0, jnp.concatenate([r[-1:], r[:-1]], 0), r)


def set_caps(fw, iw, sites):
    found = []
    for i, at in sites:

        def d_at(plane, row):
            return iw[PATTERN, plane, :, pl.ds(row, T), :]

        d = d_at(i, at)
        others = (x_next(d), x_prev(d), d_at(i, at + 1), d_at(i, at - 1), d_at(i + 1, at), d_at(i - 1, at))
        found.append([(d & (1 << j)) | (other & (1 << (j ^ 1))) for j, other in enumerate(others)])
    caps = [[jnp.where(linked != 0, BIG, -3.0) for linked in some] for some in found]
    for (i, at), some in zip(sites, caps):
        for j, cap in enumerate(some):
            fw[CAPS + j, i, :, pl.ds(at, T), :] = cap
    return caps


def caps_of(fw, sites):
    return [[fw[CAPS + j, i, :, pl.ds(at, T), :] for j in range(6)] for i, at in sites]


def select(fw, iw, step, sites, caps):
    found = []
    for (i, at), cap in zip(sites, caps):

        def p_at(plane, row):
            return fw[STATE + step, plane, :, pl.ds(row, T), :]

        p = p_at(i, at)
        y = jnp.maximum(jnp.minimum(p_at(i, at + 1), cap[2]), jnp.minimum(p_at(i, at - 1), cap[3]))
        z = jnp.maximum(jnp.minimum(p_at(i + 1, at), cap[4]), jnp.minimum(p_at(i - 1, at), cap[5]))
        x = jnp.maximum(jnp.minimum(x_next(p), cap[0]), jnp.minimum(x_prev(p), cap[1]))
        found.append((p >= 0) & (p > jnp.maximum(jnp.maximum(y, z), x)))
    for (i, at), new in zip(sites, found):
        iw[NEW + 1 + step, i, :, pl.ds(at, T), :] = jnp.where(new, 63, 0)


def hits(fw, iw, step, i, at):
    def n_at(plane, row):
        return iw[NEW + 1 + step, plane, :, pl.ds(row, T), :]

    new = n_at(i, at)
    hit = ((n_at(i, at + 1) & 4) | (n_at(i, at - 1) & 8)) | ((n_at(i + 1, at) & 16) | (n_at(i - 1, at) & 32))
    hit |= (x_next(new) & 1) | (x_prev(new) & 2)
    hit &= iw[PATTERN, i, :, pl.ds(at, T), :]
    return new != 0, hit != 0, fw[STATE + step, i, :, pl.ds(at, T), :]


def update(fw, iw, step, sites):
    found = []
    for i, at in sites:
        new, hit, p = hits(fw, iw, step, i, at)
        found.append(jnp.where(new, -2.0, jnp.where((p >= 0) & hit, -1.0, p)))
    for (i, at), p in zip(sites, found):
        fw[STATE + step + 1, i, :, pl.ds(at, T), :] = p


def stages(fw, iw, depth, rows_of):
    for stage in range(2 * ROUNDS - 1):
        step, reach = stage // 2, H - 1 - stage

        def planes(i, each):
            sites = [(i + j, at) for j in range(each) for at in rows_of(stage)]
            if stage == 0:
                select(fw, iw, step, sites, set_caps(fw, iw, sites))
            elif stage % 2 == 0:
                select(fw, iw, step, sites, caps_of(fw, sites))
            else:
                update(fw, iw, step, sites)

        first, count = H - reach, depth + 2 * reach
        each = 3 if stage == 0 and count % 3 == 0 else 4
        whole_steps = count // each * each

        @pl.loop(first, first + whole_steps, step=each)
        def _(i):
            planes(i, each)

        if count > whole_steps:
            planes(first + whole_steps, count - whole_steps)


def inner_kernel(d_ext, m_ext, fw, iw):
    planes, rows, _ = m_ext.shape
    depth = planes - 2 * H

    @pl.loop(0, planes)
    def _(i):
        iw[PATTERN, i, :, pl.ds(T, rows), :] = blocks(d_ext[i])
        fw[STATE, i, :, pl.ds(T, rows), :] = blocks(m_ext[i])

    stages(fw, iw, depth, lambda stage: range(T, T + rows, T))


def outer_kernel(ro1, re1, ro2, re2, fw_in, iw_in, state_out, count_out, fw, iw, state_ref, sems):
    del fw_in, iw_in
    depth, rows, width = state_ref.shape
    planes = depth + 2 * H
    ylo, yhi = neighbours("gy")
    even = lax.axis_index("gy") % 2 == 0

    def unpack(above, below, early):
        patterns, measures, _ = y_layout(depth, early)
        for z, n, at in patterns:
            d = jnp.where(yhi, above[pl.ds(at, n), :], 0.0).astype(I32)
            iw[PATTERN, z + H, :, pl.ds(T + rows, n), :] = blocks(d)
            d = jnp.where(ylo, below[pl.ds(at, n), :], 0.0).astype(I32)
            iw[PATTERN, z + H, :, pl.ds(T - n, n), :] = blocks(d)
        for z, n, at in measures:
            fw[STATE, z + H, :, pl.ds(T + rows, n), :] = blocks(above[pl.ds(at, n), :])
            fw[STATE, z + H, :, pl.ds(T - n, n), :] = blocks(below[pl.ds(at, n), :])

    @pl.when(even)
    def _():
        unpack(re1, ro1, True)
        unpack(re2, ro2, False)

    @pl.when(jnp.logical_not(even))
    def _():
        unpack(ro1, re1, True)
        unpack(ro2, re2, False)

    def low(stage):
        return T - H + stage

    def high(stage):
        return T + rows + H - T - stage

    shape = (width // L, T, L)
    row = lax.broadcasted_iota(I32, shape, 1)

    each = max(n for n in (1, 2, 4) if planes % n == 0)

    @pl.loop(0, planes, step=each)
    def _(i):
        sites = [(i + j, *edge) for j in range(each) for edge in ((low(0), H - 1, H), (high(0), T - H - 1, T - H))]
        found = []
        for i, at, one, two in sites:
            d_next = iw[PATTERN, i, :, pl.ds(at + 1, T), :]
            d_prev = iw[PATTERN, i, :, pl.ds(at - 1, T), :]
            bit = jnp.where(row == one, d_next & 8, jnp.where(row == two, d_prev & 4, 0))
            found.append(scaled(fw[STATE, i, :, pl.ds(at, T), :], bit))
        for (i, at, _, _), p in zip(sites, found):
            fw[STATE, i, :, pl.ds(at, T), :] = p

    stages(fw, iw, depth, lambda stage: (low(stage), high(stage)))

    def finish(z, totals):
        totals = list(totals)
        for at in range(0, rows, T):
            new, hit, p = hits(fw, iw, ROUNDS - 1, z + H, T + at)
            old = jnp.where(p >= 0, jnp.where(hit, 1, 0), jnp.where(p == -2.0, 2, 1))
            state = jnp.where(new, 2, old)
            for j in range(width // L):
                state_ref[z, pl.ds(at, T), pl.ds(j * L, L)] = state[j]
            totals[-1] = totals[-1] + jnp.where(state == 0, 1, 0)
            for step in range(ROUNDS - 1):
                p = fw[STATE + step + 1, z + H, :, pl.ds(T + at, T), :]
                totals[step] = totals[step] + jnp.where(p >= 0, 1, 0)
        pltpu.make_async_copy(state_ref.at[z], state_out.at[z], sems.at[z]).start()
        return tuple(totals)

    totals = lax.fori_loop(0, depth, finish, (jnp.zeros(shape, I32),) * ROUNDS, unroll=2 - depth % 2)
    row = lax.broadcasted_iota(I32, (T, L), 0)
    lane = lax.broadcasted_iota(I32, (T, L), 1)
    partial = jnp.zeros((T, L), I32)
    for step in range(ROUNDS):
        partial = jnp.where(row == step, jnp.sum(jnp.sum(totals[step], axis=0), axis=0, keepdims=True), partial)
    counts = jnp.where(lane == row, jnp.sum(partial, axis=1, keepdims=True), 0)
    counts = jnp.sum(counts, axis=0, keepdims=True)
    count_out[...] = jnp.broadcast_to(counts[None], count_out.shape)
    for z in range(depth):
        pltpu.make_async_copy(state_ref.at[z], state_out.at[z], sems.at[z]).wait()


def shift(value, axis, step):
    count = lax.axis_size(axis)
    return lax.ppermute(value, axis, [(i, (i + step) % count) for i in range(count)])


def swap(value, axis, odd):
    count = lax.axis_size(axis)
    pairs = [(i, i) for i in range(count)]
    for i in range(odd, count - 1, 2):
        pairs[i], pairs[i + 1] = (i, i + 1), (i + 1, i)
    return lax.ppermute(value, axis, pairs)


def relay(value, axis):
    last = lax.axis_size(axis) - 1
    pairs = [(i, min(i + 2, last) if i % 2 == 0 else max(i - 2, 0)) for i in range(last + 1)]
    return lax.ppermute(value, axis, pairs)


def call(kernel, outs, args, limit, cost, **more):
    return pl.pallas_call(
        kernel,
        out_shape=outs,
        in_specs=[vmem()] * len(args),
        out_specs=more.pop("out_specs", [vmem()] * len(outs)),
        compiler_params=pltpu.CompilerParams(vmem_limit_bytes=limit * 2**20),
        cost_estimate=pl.CostEstimate(flops=cost, bytes_accessed=cost, transcendentals=0),
        **more,
    )(*args)


def per_device(ranks, seeds, flags):
    depth, rows, width = ranks.shape
    assert RELAYED <= 2 * H - depth and H < depth and lax.axis_size("gz") % 2 == 0 and rows >= 2 * T and T == H + 2 and width % L == 0
    planes = depth + 2 * H
    devices = lax.axis_size("gz") * lax.axis_size("gy")
    of = jax.ShapeDtypeStruct
    own = [of(ranks.shape, F32)]
    sz_top, sy_last, twice, rm = call(
        edge_kernel,
        [of((rows, width), F32), of((depth, width), F32), of(seeds.shape, F32)] + own,
        (seeds,),
        8,
        4000000,
    )
    sy_low = shift(sy_last, "gy", 1)
    sz_low = shift(sz_top, "gz", 1)
    packed = jnp.where(flags == 0, ranks, jnp.where(flags == 2, -2.0, -1.0))
    messages = [of((2 * len(zs) * rows, width), F32) for zs in plane_lists(depth)]
    cells = [of(ranks.shape, I32)] + own
    scratch = [pltpu.VMEM(ranks.shape, I32), pltpu.VMEM(ranks.shape, F32)]
    (both,) = call(shared_kernel, messages[:1], (twice, rm, packed, sy_low), 8, 4000000, scratch_shapes=scratch)
    both = swap(both, "gz", 0)
    partner, other, d_own, m_own = call(
        strength_kernel, messages[1:] + cells, (twice, rm, packed, sz_low, sy_low), 8, 4000000
    )
    partner = swap(partner, "gz", 0)
    relayed = relay(both, "gz")
    other = swap(other, "gz", 1)
    message = of((y_layout(depth, True)[2], width), F32)
    yo, ye = call(early_kernel, [message, message], (d_own, m_own), 8, 1000000)
    ro1 = swap(yo, "gy", 1)
    re1 = swap(ye, "gy", 0)
    message = of((y_layout(depth, False)[2], width), F32)
    ext = (planes, rows, width)
    yo, ye, d_ext, m_ext = call(
        planes_kernel, [message, message, of(ext, I32), of(ext, F32)], (both, partner, other, relayed, d_own, m_own), 8, 4000000
    )
    ro2 = swap(yo, "gy", 1)
    re2 = swap(ye, "gy", 0)
    cells = (planes, width // L, rows + 2 * T, L)
    works = [of((STATE + ROUNDS,) + cells, F32), of((NEW + 1 + ROUNDS,) + cells, I32)]
    fw, iw = call(inner_kernel, works, (d_ext, m_ext), 8, 20000000)
    state, counts, _, _ = call(
        outer_kernel,
        [of(ranks.shape, I32), of((devices, 1, L), I32)] + works,
        (ro1, re1, ro2, re2, fw, iw),
        8,
        20000000,
        input_output_aliases={4: 2, 5: 3},
        out_specs=[pl.BlockSpec(memory_space=pl.ANY), vmem(), vmem(), vmem()],
        scratch_shapes=[pltpu.VMEM(ranks.shape, I32), pltpu.SemaphoreType.DMA((depth,))],
    )
    everyone = lax.all_to_all(counts, ("gz", "gy"), 0, 0, tiled=True)
    undecided = jnp.sum(everyone, axis=(0, 1))[:ROUNDS]
    return (state, undecided)


def solution(mesh):
    return jax.shard_map(
        per_device,
        mesh=mesh,
        in_specs=(P("gz", "gy", None), P(None, "gz", "gy", None), P("gz", "gy", None)),
        out_specs=(P("gz", "gy", None), P()),
        check_vma=False,
    )
```
